8 devices in a mesh: pp: 4 (over z, y, x), dp: 2 (over core).
Axes of the slice: x: 2, y: 2, z: 1, core: 2. Of those that a mesh axis runs over, the one named last changes fastest.
Arguments:
- tok_ids: int32 [4, 1024], P(None, 'dp')
- d_out: bfloat16 [4, 1024, 128], P('pp', 'dp')
- stored_x: bfloat16 [4, 4, 1024, 128], P('pp', None, 'dp')
- w_in: bfloat16 [32, 128, 512], P('pp')
- w_out: bfloat16 [32, 512, 128], P('pp')
- acc_in: float32 [32, 2, 128, 512], P('pp', 'dp')
- acc_out: float32 [32, 2, 512, 128], P('pp', 'dp')
- acc_emb: float32 [2, 30522, 128], P('dp')
Outputs:
- output 1: float32 [32, 128, 512], P('pp', 'dp')
- output 2: float32 [32, 512, 128], P('pp', 'dp')
- output 3: float32 [30522, 128], P(None, 'dp')
All inputs are finite; a program needn't handle non-finite values.
Results may differ from the reference program's by a relative error of at most 0.016148.
Values are sent between devices in bfloat16 or wider.
A program may use at most 1 GiB of HBM per device.

```python
import jax
import jax.numpy as jnp
from jax import lax

STAGES = 4
REPLICAS = 2
LAYERS = 8
HID = 128
FF = 512
VOCAB = 30522
TOKENS_DEV = 512

ROWS_ALL = TOKENS_DEV * REPLICAS


def setup_inputs(seed: int = 0) -> dict:
    key_list = jax.random.split(jax.random.key(seed), 8)
    tok_ids = jax.random.randint(key_list[0], (STAGES, ROWS_ALL), 0, VOCAB, dtype=jnp.int32)
    d_out = jax.random.normal(key_list[1], (STAGES, ROWS_ALL, HID), jnp.float32).astype(jnp.bfloat16)
    stored_x = jax.random.normal(key_list[2], (STAGES, STAGES, ROWS_ALL, HID), jnp.float32).astype(jnp.bfloat16)
    w_in = (jax.random.normal(key_list[3], (STAGES * LAYERS, HID, FF), jnp.float32) * HID ** -0.5).astype(jnp.bfloat16)
    w_out = (jax.random.normal(key_list[4], (STAGES * LAYERS, FF, HID), jnp.float32) * (FF * STAGES * LAYERS) ** -0.5).astype(jnp.bfloat16)
    in_scale = 0.2 * (TOKENS_DEV / LAYERS) ** 0.5
    out_scale = 0.4 * (TOKENS_DEV * STAGES) ** 0.5
    acc_in = jax.random.normal(key_list[5], (STAGES * LAYERS, REPLICAS, HID, FF), jnp.float32) * in_scale
    acc_out = jax.random.normal(key_list[6], (STAGES * LAYERS, REPLICAS, FF, HID), jnp.float32) * out_scale
    acc_emb = jax.random.normal(key_list[7], (REPLICAS, VOCAB, HID), jnp.float32) * 0.5
    return {'tok_ids': tok_ids, 'd_out': d_out, 'stored_x': stored_x, 'w_in': w_in, 'w_out': w_out, 'acc_in': acc_in, 'acc_out': acc_out, 'acc_emb': acc_emb}


def layer_forward(x_cur, w_in_l, w_out_l):
    pre_act = jnp.dot(x_cur, w_in_l, preferred_element_type=jnp.float32).astype(jnp.bfloat16)
    hidden = jax.nn.gelu(pre_act.astype(jnp.float32)).astype(jnp.bfloat16)
    out_x = (x_cur.astype(jnp.float32) + jnp.dot(hidden, w_out_l, preferred_element_type=jnp.float32)).astype(jnp.bfloat16)
    return out_x, pre_act, hidden


def per_replica(left_rows, right_rows):
    left_r = left_rows.reshape(REPLICAS, TOKENS_DEV, left_rows.shape[-1]).astype(jnp.float32)
    right_r = right_rows.reshape(REPLICAS, TOKENS_DEV, right_rows.shape[-1]).astype(jnp.float32)
    return jnp.einsum('rti,rtf->rif', left_r, right_r)


def stage_backward(w_in_s, w_out_s, acc_in_s, acc_out_s, x_stage, cot_stage):
    def one_micro(carry, item):
        sum_in, sum_out = carry
        x_first, cot_first = item

        def fwd_step(x_cur, weights):
            out_x, pre_act, hidden = layer_forward(x_cur, weights[0], weights[1])
            return out_x, (x_cur, pre_act, hidden)

        _, saved_acts = lax.scan(fwd_step, x_first, (w_in_s, w_out_s))

        def bwd_step(cot_cur, layer_item):
            w_in_l, w_out_l, x_cur, pre_act, hidden = layer_item
            g_out = per_replica(hidden, cot_cur)
            d_hidden = jnp.dot(cot_cur, w_out_l.T, preferred_element_type=jnp.float32).astype(jnp.bfloat16)
            pre_f = pre_act.astype(jnp.float32)
            gelu_slope = jax.jvp(jax.nn.gelu, (pre_f,), (jnp.ones_like(pre_f),))[1]
            d_pre = (d_hidden.astype(jnp.float32) * gelu_slope).astype(jnp.bfloat16)
            g_in = per_replica(x_cur, d_pre)
            d_x = (cot_cur.astype(jnp.float32) + jnp.dot(d_pre, w_in_l.T, preferred_element_type=jnp.float32)).astype(jnp.bfloat16)
            return d_x, (g_in, g_out)

        d_first, grads = lax.scan(bwd_step, cot_first, (w_in_s, w_out_s) + saved_acts, reverse=True)
        return (sum_in + grads[0], sum_out + grads[1]), d_first

    sums, d_cots = lax.scan(one_micro, (acc_in_s, acc_out_s), (x_stage, cot_stage))
    return sums[0], sums[1], d_cots


def replica_mean(total, axis_pos):
    return jnp.sum(total.astype(jnp.bfloat16).astype(jnp.float32), axis=axis_pos) / REPLICAS


def reference(tok_ids, d_out, stored_x, w_in, w_out, acc_in, acc_out, acc_emb):
    grads_in = []
    grads_out = []
    cot_rows = d_out[:0]
    for stage_id in range(STAGES - 1, -1, -1):
        pending = STAGES - stage_id
        first_row = stage_id * LAYERS
        last_row = first_row + LAYERS
        cot_rows = jnp.concatenate([cot_rows, d_out[stage_id:stage_id + 1]], axis=0)
        sum_in, sum_out, cot_rows = stage_backward(w_in[first_row:last_row], w_out[first_row:last_row], acc_in[first_row:last_row], acc_out[first_row:last_row], stored_x[stage_id, :pending], cot_rows)
        grads_in = [replica_mean(sum_in, 1)] + grads_in
        grads_out = [replica_mean(sum_out, 1)] + grads_out
    row_replica = jnp.arange(ROWS_ALL, dtype=jnp.int32) // TOKENS_DEV
    segment_ids = (tok_ids + row_replica[None, :] * VOCAB).reshape(-1)
    emb_new = jax.ops.segment_sum(cot_rows.reshape(-1, HID).astype(jnp.float32), segment_ids, num_segments=REPLICAS * VOCAB)
    grad_emb = replica_mean(acc_emb + emb_new.reshape(REPLICAS, VOCAB, HID), 0)
    return (jnp.concatenate(grads_in, axis=0), jnp.concatenate(grads_out, axis=0), grad_emb)
```

```python
import functools

import jax
import jax.numpy as jnp
from jax import lax
from jax.experimental import pallas as pl
from jax.experimental.pallas import tpu as pltpu
from jax.sharding import PartitionSpec as P

MESH = pl.DeviceIdType.MESH
F32 = jnp.float32
BF16 = jnp.bfloat16
NT = (((1,), (1,)), ((), ()))
C0 = 0.7978845608028654
C1 = 0.7978845608028654 * 0.044715
FF_CHUNK = 256
VOCAB_BLOCK = 2048
VOCAB_TILE = 256


def gelu_parts(pre_act):
    square = pre_act * pre_act
    tanh_val = jnp.tanh(pre_act * (C0 + C1 * square))
    half = 0.5 + 0.5 * tanh_val
    value = pre_act * half
    slope = half + (value - value * half) * (2.0 * C0 + (6.0 * C1) * square)
    return value, slope


def forward_layer(layer_id, w_in, w_out, acts_x, acts_a, acts_s):
    x_cur = acts_x[layer_id]
    out_x = x_cur.astype(F32)
    for start in range(0, w_in.shape[2], FF_CHUNK):
        cols = pl.ds(start, FF_CHUNK)
        pre_act = jnp.dot(x_cur, w_in[layer_id, :, cols], preferred_element_type=F32).astype(BF16)
        value, slope = gelu_parts(pre_act.astype(F32))
        hidden = value.astype(BF16)
        acts_a[layer_id, :, cols] = hidden
        acts_s[layer_id, :, cols] = slope
        out_x += jnp.dot(hidden, w_out[layer_id, cols, :], preferred_element_type=F32)
    acts_x[layer_id + 1] = out_x.astype(BF16)


def backward_layer(layer_id, w_in, w_out, acts_x, acts_a, acts_s, cot, sum_in, sum_out_t):
    cot_cur = cot[...]
    cot_t = cot_cur.T
    x_t = acts_x[layer_id].T
    d_x = cot_cur.astype(F32)
    for start in range(0, w_in.shape[2], FF_CHUNK):
        cols = pl.ds(start, FF_CHUNK)
        d_hidden = lax.dot_general(cot_cur, w_out[layer_id, cols, :], NT, preferred_element_type=F32).astype(BF16)
        d_pre = (d_hidden.astype(F32) * acts_s[layer_id, :, cols]).astype(BF16)
        d_x += lax.dot_general(d_pre, w_in[layer_id, :, cols], NT, preferred_element_type=F32)
        sum_out_t[layer_id, :, cols] += jnp.dot(cot_t, acts_a[layer_id, :, cols], preferred_element_type=F32)
        sum_in[layer_id, :, cols] += jnp.dot(x_t, d_pre, preferred_element_type=F32)
    cot[...] = d_x.astype(BF16)


def stage_kernel(stages, ids, d_out, stored_x, w_in, w_out, acc_in, acc_out, acc_emb,
                 ids_peer, acc_peer, dx_all, gi_own, gi_recv, go_own, go_recv,
                 acts_x, acts_a, acts_s, cot, dx_send, cot_in, sum_in, sum_out_t, acc_o, gi_bf, go_bf,
                 load_sem, ex_send, ex_recv, cot_send, cot_recv, bc_send, bc_recv, pr_send, pr_recv, loc_sem, g_sem, g_send, g_recv):
    stage = lax.axis_index('pp')
    rep = lax.axis_index('dp')
    other = 1 - rep
    layers = w_in.shape[0]
    last = stages - 1

    barrier = pltpu.get_barrier_semaphore()
    for hop in range(1, 2 * stages):
        place = lax.rem(stage * 2 + rep + hop, 2 * stages)
        pl.semaphore_signal(barrier, inc=1, device_id=(place // 2, lax.rem(place, 2)), device_id_type=MESH)

    load_in = pltpu.make_async_copy(acc_in, sum_in, load_sem.at[0])
    load_out = pltpu.make_async_copy(acc_out, acc_o, load_sem.at[1])
    load_in.start()
    load_out.start()
    sum_out_t[...] = jnp.zeros_like(sum_out_t)

    def forward(step_id):
        acts_x[0] = stored_x[last - stage - step_id]
        pl.loop(0, layers)(lambda layer_id: forward_layer(layer_id, w_in, w_out, acts_x, acts_a, acts_s))

    forward(0)
    pl.semaphore_wait(barrier, 2 * stages - 1)

    ex_ids = pltpu.make_async_remote_copy(ids, ids_peer, ex_send.at[0], ex_recv.at[0], device_id=(stage, other), device_id_type=MESH)
    ex_emb = pltpu.make_async_remote_copy(acc_emb, acc_peer, ex_send.at[1], ex_recv.at[1], device_id=(stage, other), device_id_type=MESH)
    ex_ids.start()
    ex_emb.start()
    load_in.wait()
    load_out.wait()

    def cot_copy(step_id):
        return pltpu.make_async_remote_copy(dx_send.at[step_id], cot_in.at[step_id], cot_send.at[step_id], cot_recv.at[step_id],
                                            device_id=(jnp.maximum(stage - 1, 0), rep), device_id_type=MESH)

    def bc_copy(step_id, target):
        return pltpu.make_async_remote_copy(dx_send.at[step_id], dx_all.at[rep, last - step_id], bc_send.at[target, step_id], bc_recv.at[step_id],
                                            device_id=(target, rep), device_id_type=MESH)

    def peer_copy(step_id, src):
        return pltpu.make_async_remote_copy(src, dx_all.at[rep, last - step_id], pr_send.at[step_id], pr_recv.at[step_id],
                                            device_id=(stage, other), device_id_type=MESH)

    def local_copy(step_id):
        return pltpu.make_async_copy(dx_send.at[step_id], dx_all.at[rep, last - step_id], loc_sem.at[step_id])

    @pl.loop(0, stages)
    def _(step_id):
        @pl.when(stage + step_id <= last)
        def _():
            @pl.when(step_id == 0)
            def _():
                cot[...] = d_out[...]

            @pl.when(step_id > 0)
            def _():
                forward(step_id)
                cot_copy(step_id - 1).wait_recv()
                cot[...] = cot_in[step_id - 1]

            pl.loop(0, layers)(lambda back_id: backward_layer(layers - 1 - back_id, w_in, w_out, acts_x, acts_a, acts_s, cot, sum_in, sum_out_t))
            dx_send[step_id] = cot[...]

            @pl.when(stage > 0)
            def _():
                cot_copy(step_id).start()

            @pl.when(stage == 0)
            def _():
                for target in range(1, stages):
                    bc_copy(step_id, target).start()
                peer_copy(step_id, dx_send.at[step_id]).start()
                local_copy(step_id).start()

    @pl.loop(0, layers)
    def _(layer_id):
        gi_bf[layer_id] = sum_in[layer_id].astype(BF16)
        go_bf[layer_id] = (sum_out_t[layer_id].T + acc_o[layer_id]).astype(BF16)

    half_i = gi_own.shape[1]
    half_o = go_own.shape[1]
    keep = [
        pltpu.make_async_copy(gi_bf.at[:, pl.ds(pl.multiple_of(rep * half_i, half_i), half_i), :], gi_own, g_sem.at[0]),
        pltpu.make_async_copy(go_bf.at[:, pl.ds(pl.multiple_of(rep * half_o, half_o), half_o), :], go_own, g_sem.at[1]),
    ]
    give = [
        pltpu.make_async_remote_copy(gi_bf.at[:, pl.ds(pl.multiple_of(other * half_i, half_i), half_i), :], gi_recv, g_send.at[0], g_recv.at[0], device_id=(stage, other), device_id_type=MESH),
        pltpu.make_async_remote_copy(go_bf.at[:, pl.ds(pl.multiple_of(other * half_o, half_o), half_o), :], go_recv, g_send.at[1], g_recv.at[1], device_id=(stage, other), device_id_type=MESH),
    ]
    for copy in keep + give:
        copy.start()

    @pl.when(stage > 0)
    def _():
        for step_id in range(stages):
            bc_copy(step_id, 0).wait_recv()
            peer_copy(step_id, dx_all.at[rep, last - step_id]).start()
        for step_id in range(stages):
            @pl.when(stage + step_id <= last)
            def _():
                cot_copy(step_id).wait_send()

    @pl.when(stage == 0)
    def _():
        for step_id in range(stages):
            for target in range(1, stages):
                bc_copy(step_id, target).wait_send()
            local_copy(step_id).wait()

    for step_id in range(stages):
        peer_copy(step_id, dx_send.at[step_id]).wait()
    for copy in keep + give:
        copy.wait()
    ex_ids.wait()
    ex_emb.wait()


def finish_kernel(vocab, ids_own, ids_peer, acc_own, acc_peer, dx_all, gi_own, gi_recv, go_own, go_recv,
                  emb_t, grad_in, grad_out, tab_own, tab_peer, dxf, sems):
    step = pl.program_id(0)
    rep = lax.axis_index('dp')
    padded = tab_own.shape[0]
    rows_own = tab_own.reshape(padded, tab_own.shape[2])
    rows_peer = tab_peer.reshape(padded, tab_peer.shape[2])
    micros, tokens = ids_own.shape

    @pl.when(step == 0)
    def _():
        load_own = pltpu.make_async_copy(acc_own, tab_own.at[pl.ds(0, vocab)], sems.at[0])
        load_peer = pltpu.make_async_copy(acc_peer, tab_peer.at[pl.ds(0, vocab)], sems.at[1])
        load_own.start()
        load_peer.start()
        grad_in[...] = (gi_own[...].astype(F32) + gi_recv[...].astype(F32)) * 0.5
        grad_out[...] = (go_own[...].astype(F32) + go_recv[...].astype(F32)) * 0.5
        dxf[0] = dx_all[rep].astype(F32)
        dxf[1] = dx_all[1 - rep].astype(F32)
        load_own.wait()
        load_peer.wait()
        for micro in range(micros):
            def add_rows(row, carry):
                first = ids_own[micro, row]
                second = ids_peer[micro, row]
                rows_own[pl.ds(first, 1), :] = rows_own[pl.ds(first, 1), :] + dxf[0, micro, pl.ds(row, 1), :]
                rows_peer[pl.ds(second, 1), :] = rows_peer[pl.ds(second, 1), :] + dxf[1, micro, pl.ds(row, 1), :]
                return carry
            lax.fori_loop(0, tokens, add_rows, 0, unroll=8)

    half = emb_t.shape[0]
    width = tab_own.shape[2]
    row_id = lax.broadcasted_iota(jnp.int32, (half, 2 * width), 0)
    col_id = lax.broadcasted_iota(jnp.int32, (half, 2 * width), 1)
    pick = jnp.where(lax.rem(col_id, width) == row_id + half * rep, 0.5, 0.0).astype(BF16)
    for start in range(0, emb_t.shape[1], VOCAB_TILE):
        first = pl.multiple_of(step * emb_t.shape[1] + start, 8)
        both = jnp.concatenate([rows_own[pl.ds(first, VOCAB_TILE), :].astype(BF16), rows_peer[pl.ds(first, VOCAB_TILE), :].astype(BF16)], axis=1)
        emb_t[:, start:start + VOCAB_TILE] = lax.dot_general(pick, both, NT, preferred_element_type=F32)


def solution(mesh):
    stages = mesh.shape['pp']

    def device_body(tok_ids, d_out, stored_x, w_in, w_out, acc_in, acc_out, acc_emb):
        layers, hid, ff = w_in.shape
        tokens = d_out.shape[1]
        vocab = acc_emb.shape[1]
        half_i, half_o, half_e = hid // 2, ff // 2, hid // 2
        emb_rows = acc_emb.reshape(vocab, 1, hid)
        any_spec = pl.BlockSpec(memory_space=pl.ANY)
        vmem_spec = pl.BlockSpec(memory_space=pltpu.VMEM)
        dma = pltpu.SemaphoreType.DMA
        ids_peer, acc_peer, dx_all, gi_own, gi_recv, go_own, go_recv = pl.pallas_call(
            functools.partial(stage_kernel, stages),
            name='stage_pipeline',
            in_specs=[any_spec] + [vmem_spec] * 4 + [any_spec] * 3,
            out_specs=[any_spec] * 7,
            out_shape=[
                jax.ShapeDtypeStruct(tok_ids.shape, tok_ids.dtype),
                jax.ShapeDtypeStruct((vocab, 1, hid), F32),
                jax.ShapeDtypeStruct((2, stages, tokens, hid), BF16),
                jax.ShapeDtypeStruct((layers, half_i, ff), BF16),
                jax.ShapeDtypeStruct((layers, half_i, ff), BF16),
                jax.ShapeDtypeStruct((layers, half_o, hid), BF16),
                jax.ShapeDtypeStruct((layers, half_o, hid), BF16),
            ],
            scratch_shapes=[
                pltpu.VMEM((layers + 1, tokens, hid), BF16),
                pltpu.VMEM((layers, tokens, ff), BF16),
                pltpu.VMEM((layers, tokens, ff), F32),
                pltpu.VMEM((tokens, hid), BF16),
                pltpu.VMEM((stages, tokens, hid), BF16),
                pltpu.VMEM((stages, tokens, hid), BF16),
                pltpu.VMEM((layers, hid, ff), F32),
                pltpu.VMEM((layers, hid, ff), F32),
                pltpu.VMEM((layers, ff, hid), F32),
                pltpu.VMEM((layers, hid, ff), BF16),
                pltpu.VMEM((layers, ff, hid), BF16),
                dma((2,)), dma((2,)), dma((2,)),
                dma((stages,)), dma((stages,)),
                dma((stages, stages)), dma((stages,)),
                dma((stages,)), dma((stages,)), dma((stages,)),
                dma((2,)), dma((2,)), dma((2,)),
            ],
            compiler_params=pltpu.CompilerParams(collective_id=0, has_side_effects=True, vmem_limit_bytes=60 * 2**20),
        )(tok_ids, d_out[0], stored_x[0], w_in, w_out, acc_in[:, 0], acc_out[:, 0], emb_rows)

        padded = pl.cdiv(vocab, VOCAB_BLOCK) * VOCAB_BLOCK
        whole = lambda shape: pl.BlockSpec(shape, lambda step: (0,) * len(shape))
        smem_spec = pl.BlockSpec(memory_space=pltpu.SMEM)
        emb_t, grad_in, grad_out = pl.pallas_call(
            functools.partial(finish_kernel, vocab),
            name='finish',
            grid=(pl.cdiv(vocab, VOCAB_BLOCK),),
            in_specs=[smem_spec] * 2 + [any_spec] * 2 + [whole(v.shape) for v in (dx_all, gi_own, gi_recv, go_own, go_recv)],
            out_specs=[pl.BlockSpec((half_e, VOCAB_BLOCK), lambda step: (0, step)), whole((layers, half_i, ff)), whole((layers, half_o, hid))],
            out_shape=[
                jax.ShapeDtypeStruct((half_e, vocab), F32),
                jax.ShapeDtypeStruct((layers, half_i, ff), F32),
                jax.ShapeDtypeStruct((layers, half_o, hid), F32),
            ],
            scratch_shapes=[
                pltpu.VMEM((padded, 1, hid), F32),
                pltpu.VMEM((padded, 1, hid), F32),
                pltpu.VMEM((2, stages, tokens, hid), F32),
                dma((2,)),
            ],
            compiler_params=pltpu.CompilerParams(vmem_limit_bytes=60 * 2**20),
        )(tok_ids, ids_peer, emb_rows, acc_peer, dx_all, gi_own, gi_recv, go_own, go_recv)
        return grad_in, grad_out, emb_t.T

    return jax.shard_map(device_body, mesh=mesh, in_specs=(P(None, 'dp'), P('pp', 'dp', None), P('pp', None, 'dp', None), P('pp', None, None), P('pp', None, None), P('pp', 'dp', None, None), P('pp', 'dp', None, None), P('dp', None, None)), out_specs=(P('pp', 'dp', None), P('pp', 'dp', None), P(None, 'dp')), check_vma=False)
```

```python
import functools

import jax
import jax.numpy as jnp
from jax import lax
from jax.experimental import pallas as pl
from jax.experimental.pallas import tpu as pltpu
from jax.sharding import PartitionSpec as P

MESH = pl.DeviceIdType.MESH
F32 = jnp.float32
BF16 = jnp.bfloat16
NT = (((1,), (1,)), ((), ()))
C0 = 0.7978845608028654
C1 = 0.7978845608028654 * 0.044715
FF_CHUNK = 256
GROUP = 8
VOCAB_BLOCK = 2048
VOCAB_TILE = 256


def gelu_parts(pre_act):
    square = pre_act * pre_act
    tanh_val = jnp.tanh(pre_act * (C0 + C1 * square))
    half = 0.5 + 0.5 * tanh_val
    value = pre_act * half
    slope = half + (value - value * half) * (2.0 * C0 + (6.0 * C1) * square)
    return value, slope


def forward_layer(layer_id, w_in, w_out, acts_x, acts_a, acts_s):
    x_cur = acts_x[layer_id]
    out_x = x_cur.astype(F32)
    for start in range(0, w_in.shape[2], FF_CHUNK):
        cols = pl.ds(start, FF_CHUNK)
        pre_act = jnp.dot(x_cur, w_in[layer_id, :, cols], preferred_element_type=F32).astype(BF16)
        value, slope = gelu_parts(pre_act.astype(F32))
        hidden = value.astype(BF16)
        acts_a[layer_id, :, cols] = hidden
        acts_s[layer_id, :, cols] = slope
        out_x += jnp.dot(hidden, w_out[layer_id, cols, :], preferred_element_type=F32)
    acts_x[layer_id + 1] = out_x.astype(BF16)


def backward_layer(layer_id, w_in, w_out, acts_x, acts_a, acts_s, cot, sum_in, sum_out_t):
    cot_cur = cot[...]
    cot_t = cot_cur.T
    x_t = acts_x[layer_id].T
    d_x = cot_cur.astype(F32)
    for start in range(0, w_in.shape[2], FF_CHUNK):
        cols = pl.ds(start, FF_CHUNK)
        d_hidden = lax.dot_general(cot_cur, w_out[layer_id, cols, :], NT, preferred_element_type=F32).astype(BF16)
        d_pre = (d_hidden.astype(F32) * acts_s[layer_id, :, cols]).astype(BF16)
        d_x += lax.dot_general(d_pre, w_in[layer_id, :, cols], NT, preferred_element_type=F32)
        sum_out_t[layer_id, :, cols] += jnp.dot(cot_t, acts_a[layer_id, :, cols], preferred_element_type=F32)
        sum_in[layer_id, :, cols] += jnp.dot(x_t, d_pre, preferred_element_type=F32)
    cot[...] = d_x.astype(BF16)


def mark_repeats(ids):
    lane = lax.rem(lax.broadcasted_iota(jnp.int32, ids.shape, 1), GROUP)
    found = jnp.zeros_like(ids)
    for shift in range(1, GROUP):
        found = jnp.where((pltpu.roll(ids, shift, 1) == ids) & (lane >= shift), 1, found)
    shift = 1
    while shift < GROUP:
        found = found | pltpu.roll(found, ids.shape[1] - shift, 1)
        shift *= 2
    return found


def stage_kernel(stages, ids, d_out, stored_x, w_in, w_out, acc_in, acc_out, acc_emb,
                 marks, ids_peer, tab_own, tab_peer, dx_all, gi_own, gi_recv, go_own, go_recv,
                 acts_x, acts_a, acts_s, cot, dx_send, cot_in, sum_in, sum_out_t, acc_o, mark_own, mark_peer, ids_buf,
                 load_sem, ex_send, ex_recv, cot_send, cot_recv, bc_send, bc_recv, pr_send, pr_recv, loc_sem, g_sem, g_send, g_recv):
    stage = lax.axis_index('pp')
    rep = lax.axis_index('dp')
    other = 1 - rep
    layers = w_in.shape[0]
    last = stages - 1

    barrier = pltpu.get_barrier_semaphore()
    for hop in range(1, 2 * stages):
        place = lax.rem(stage * 2 + rep + hop, 2 * stages)
        pl.semaphore_signal(barrier, inc=1, device_id=(place // 2, lax.rem(place, 2)), device_id_type=MESH)

    load_in = pltpu.make_async_copy(acc_in, sum_in, load_sem.at[0])
    load_out = pltpu.make_async_copy(acc_out, acc_o, load_sem.at[1])
    load_in.start()
    load_out.start()
    vocab = acc_emb.shape[0]
    load_emb = pltpu.make_async_copy(acc_emb, tab_own.at[pl.ds(0, vocab)], load_sem.at[2])
    load_emb.start()
    sum_out_t[...] = jnp.zeros_like(sum_out_t)

    def forward(step_id):
        acts_x[0] = stored_x[last - stage - step_id]
        pl.loop(0, layers)(lambda layer_id: forward_layer(layer_id, w_in, w_out, acts_x, acts_a, acts_s))

    mark_own[...] = mark_repeats(ids[...])
    forward(0)
    pl.semaphore_wait(barrier, 2 * stages - 1)

    ex_ids = pltpu.make_async_remote_copy(ids, ids_buf, ex_send.at[0], ex_recv.at[0], device_id=(stage, other), device_id_type=MESH)
    ex_emb = pltpu.make_async_remote_copy(acc_emb, tab_peer.at[pl.ds(0, vocab)], ex_send.at[1], ex_recv.at[1], device_id=(stage, other), device_id_type=MESH)
    ex_ids.start()
    ex_emb.start()
    load_in.wait()
    load_out.wait()

    def cot_copy(step_id):
        return pltpu.make_async_remote_copy(dx_send.at[step_id], cot_in.at[step_id], cot_send.at[step_id], cot_recv.at[step_id],
                                            device_id=(jnp.maximum(stage - 1, 0), rep), device_id_type=MESH)

    def bc_copy(step_id, target):
        return pltpu.make_async_remote_copy(dx_send.at[step_id], dx_all.at[rep, last - step_id], bc_send.at[target, step_id], bc_recv.at[step_id],
                                            device_id=(target, rep), device_id_type=MESH)

    def peer_copy(step_id, src):
        return pltpu.make_async_remote_copy(src, dx_all.at[rep, last - step_id], pr_send.at[step_id], pr_recv.at[step_id],
                                            device_id=(stage, other), device_id_type=MESH)

    def local_copy(step_id):
        return pltpu.make_async_copy(dx_send.at[step_id], dx_all.at[rep, last - step_id], loc_sem.at[step_id])

    @pl.loop(0, stages)
    def _(step_id):
        @pl.when(stage + step_id <= last)
        def _():
            @pl.when(step_id == 0)
            def _():
                cot[...] = d_out[...]

            @pl.when(step_id > 0)
            def _():
                forward(step_id)
                cot_copy(step_id - 1).wait_recv()
                cot[...] = cot_in[step_id - 1]

            pl.loop(0, layers)(lambda back_id: backward_layer(layers - 1 - back_id, w_in, w_out, acts_x, acts_a, acts_s, cot, sum_in, sum_out_t))
            dx_send[step_id] = cot[...]

            @pl.when(stage > 0)
            def _():
                cot_copy(step_id).start()

            @pl.when(stage == 0)
            def _():
                for target in range(1, stages):
                    bc_copy(step_id, target).start()
                peer_copy(step_id, dx_send.at[step_id]).start()
                local_copy(step_id).start()

    ex_ids.wait()
    mark_peer[...] = mark_own[...] | mark_repeats(ids_buf[...])
    small = [
        pltpu.make_async_copy(mark_peer, marks, load_sem.at[3]),
        pltpu.make_async_copy(ids_buf, ids_peer, load_sem.at[4]),
    ]
    for copy in small:
        copy.start()

    gi_bf = acts_a.at[:, pl.ds(0, w_in.shape[1]), :]
    go_bf = acts_x.at[pl.ds(0, layers)]

    @pl.loop(0, layers)
    def _(layer_id):
        gi_bf[layer_id] = sum_in[layer_id].astype(BF16)
        go_bf[layer_id] = (sum_out_t[layer_id].T + acc_o[layer_id]).astype(BF16)

    half_i = gi_own.shape[1]
    half_o = go_own.shape[1]
    keep = [
        pltpu.make_async_copy(gi_bf.at[:, pl.ds(pl.multiple_of(rep * half_i, half_i), half_i), :], gi_own, g_sem.at[0]),
        pltpu.make_async_copy(go_bf.at[:, pl.ds(pl.multiple_of(rep * half_o, half_o), half_o), :], go_own, g_sem.at[1]),
    ]
    give = [
        pltpu.make_async_remote_copy(gi_bf.at[:, pl.ds(pl.multiple_of(other * half_i, half_i), half_i), :], gi_recv, g_send.at[0], g_recv.at[0], device_id=(stage, other), device_id_type=MESH),
        pltpu.make_async_remote_copy(go_bf.at[:, pl.ds(pl.multiple_of(other * half_o, half_o), half_o), :], go_recv, g_send.at[1], g_recv.at[1], device_id=(stage, other), device_id_type=MESH),
    ]
    for copy in keep + give:
        copy.start()

    @pl.when(stage > 0)
    def _():
        for step_id in range(stages):
            bc_copy(step_id, 0).wait_recv()
            peer_copy(step_id, dx_all.at[rep, last - step_id]).start()
        for step_id in range(stages):
            @pl.when(stage + step_id <= last)
            def _():
                cot_copy(step_id).wait_send()

    @pl.when(stage == 0)
    def _():
        for step_id in range(stages):
            for target in range(1, stages):
                bc_copy(step_id, target).wait_send()
            local_copy(step_id).wait()

    for step_id in range(stages):
        peer_copy(step_id, dx_send.at[step_id]).wait()
    for copy in keep + give:
        copy.wait()
    for copy in small:
        copy.wait()
    ex_emb.wait()
    load_emb.wait()


def finish_kernel(ids_own, ids_peer, marks, tab_own, tab_peer, dx_all, gi_own, gi_recv, go_own, go_recv,
                  emb_t, grad_in, grad_out, dxb, dxf, gi_buf, go_buf, gi_out, go_out, sems):
    step = pl.program_id(0)
    rep = lax.axis_index('dp')
    padded = tab_own.shape[0]
    width = tab_own.shape[2]
    rows_own = tab_own.reshape(padded, width)
    rows_peer = tab_peer.reshape(padded, width)
    micros, tokens = ids_own.shape
    load_dx = pltpu.make_async_copy(dx_all, dxb, sems.at[0])
    loads = [pltpu.make_async_copy(src, dst, sems.at[1 + pos]) for pos, (src, dst) in enumerate(
        ((gi_own, gi_buf.at[0]), (gi_recv, gi_buf.at[1]), (go_own, go_buf.at[0]), (go_recv, go_buf.at[1])))]
    stores = [pltpu.make_async_copy(gi_out, grad_in, sems.at[5]), pltpu.make_async_copy(go_out, grad_out, sems.at[6])]

    @pl.when(step == 0)
    def _():
        load_dx.start()
        for copy in loads:
            copy.start()
        load_dx.wait()
        dxf[0] = dxb[rep].astype(F32)
        dxf[1] = dxb[1 - rep].astype(F32)
        tables = ((ids_own, rows_own, 0), (ids_peer, rows_peer, 1))
        for micro in range(micros):
            def add_group(group, carry):
                base = pl.multiple_of(group * GROUP, GROUP)
                repeated = marks[micro, base] != 0

                @pl.when(repeated)
                def _():
                    for ids, rows, side in tables:
                        for pos in range(GROUP):
                            row = ids[micro, base + pos]
                            rows[pl.ds(row, 1), :] = rows[pl.ds(row, 1), :] + dxf[side, micro, pl.ds(base + pos, 1), :]

                @pl.when(jnp.logical_not(repeated))
                def _():
                    for ids, rows, side in tables:
                        places = [ids[micro, base + pos] for pos in range(GROUP)]
                        sums = [rows[pl.ds(places[pos], 1), :] + dxf[side, micro, pl.ds(base + pos, 1), :] for pos in range(GROUP)]
                        for pos in range(GROUP):
                            rows[pl.ds(places[pos], 1), :] = sums[pos]
                return carry
            lax.fori_loop(0, tokens // GROUP, add_group, 0)
        for copy in loads:
            copy.wait()
        gi_out[...] = (gi_buf[0].astype(F32) + gi_buf[1].astype(F32)) * 0.5
        go_out[...] = (go_buf[0].astype(F32) + go_buf[1].astype(F32)) * 0.5
        for copy in stores:
            copy.start()

    half = emb_t.shape[0]
    row_id = lax.broadcasted_iota(jnp.int32, (half, 2 * width), 0)
    col_id = lax.broadcasted_iota(jnp.int32, (half, 2 * width), 1)
    pick = jnp.where(lax.rem(col_id, width) == row_id + half * rep, 0.5, 0.0).astype(BF16)
    for start in range(0, emb_t.shape[1], VOCAB_TILE):
        first = pl.multiple_of(step * emb_t.shape[1] + start, 8)
        both = jnp.concatenate([rows_own[pl.ds(first, VOCAB_TILE), :].astype(BF16), rows_peer[pl.ds(first, VOCAB_TILE), :].astype(BF16)], axis=1)
        emb_t[:, start:start + VOCAB_TILE] = lax.dot_general(pick, both, NT, preferred_element_type=F32)

    @pl.when(step == pl.num_programs(0) - 1)
    def _():
        for copy in stores:
            copy.wait()


def solution(mesh):
    stages = mesh.shape['pp']

    def device_body(tok_ids, d_out, stored_x, w_in, w_out, acc_in, acc_out, acc_emb):
        layers, hid, ff = w_in.shape
        tokens = d_out.shape[1]
        vocab = acc_emb.shape[1]
        half_i, half_o, half_e = hid // 2, ff // 2, hid // 2
        emb_rows = acc_emb.reshape(vocab, 1, hid)
        table = pltpu.VMEM((pl.cdiv(vocab, VOCAB_BLOCK) * VOCAB_BLOCK, 1, hid), F32)
        any_spec = pl.BlockSpec(memory_space=pltpu.HBM)
        vmem_spec = pl.BlockSpec(memory_space=pltpu.VMEM)
        dma = pltpu.SemaphoreType.DMA
        marks, ids_peer, tab_own, tab_peer, dx_all, gi_own, gi_recv, go_own, go_recv = pl.pallas_call(
            functools.partial(stage_kernel, stages),
            name='stage_pipeline',
            in_specs=[vmem_spec] * 5 + [any_spec] * 3,
            out_specs=[any_spec] * 2 + [vmem_spec] * 2 + [any_spec] * 5,
            out_shape=[
                jax.ShapeDtypeStruct(tok_ids.shape, tok_ids.dtype),
                jax.ShapeDtypeStruct(tok_ids.shape, tok_ids.dtype),
                table,
                table,
                jax.ShapeDtypeStruct((2, stages, tokens, hid), BF16),
                jax.ShapeDtypeStruct((layers, half_i, ff), BF16),
                jax.ShapeDtypeStruct((layers, half_i, ff), BF16),
                jax.ShapeDtypeStruct((layers, half_o, hid), BF16),
                jax.ShapeDtypeStruct((layers, half_o, hid), BF16),
            ],
            scratch_shapes=[
                pltpu.VMEM((layers + 1, tokens, hid), BF16),
                pltpu.VMEM((layers, tokens, ff), BF16),
                pltpu.VMEM((layers, tokens, ff), F32),
                pltpu.VMEM((tokens, hid), BF16),
                pltpu.VMEM((stages, tokens, hid), BF16),
                pltpu.VMEM((stages, tokens, hid), BF16),
                pltpu.VMEM((layers, hid, ff), F32),
                pltpu.VMEM((layers, hid, ff), F32),
                pltpu.VMEM((layers, ff, hid), F32),
                pltpu.VMEM(tok_ids.shape, jnp.int32),
                pltpu.VMEM(tok_ids.shape, jnp.int32),
                pltpu.VMEM(tok_ids.shape, jnp.int32),
                dma((5,)), dma((2,)), dma((2,)),
                dma((stages,)), dma((stages,)),
                dma((stages, stages)), dma((stages,)),
                dma((stages,)), dma((stages,)), dma((stages,)),
                dma((2,)), dma((2,)), dma((2,)),
            ],
            compiler_params=pltpu.CompilerParams(collective_id=0, has_side_effects=True, vmem_limit_bytes=28 * 2**20),
        )(tok_ids, d_out[0], stored_x[0], w_in, w_out, acc_in[:, 0], acc_out[:, 0], emb_rows)

        resident = lambda x: pltpu.with_memory_space_constraint(x, pltpu.VMEM)
        smem_spec = pl.BlockSpec(memory_space=pltpu.SMEM)
        emb_t, grad_in, grad_out = pl.pallas_call(
            finish_kernel,
            name='finish',
            grid=(pl.cdiv(vocab, VOCAB_BLOCK),),
            in_specs=[smem_spec] * 3 + [vmem_spec] * 2 + [any_spec] * 5,
            out_specs=[pl.BlockSpec((half_e, VOCAB_BLOCK), lambda step: (0, step))] + [any_spec] * 2,
            out_shape=[
                jax.ShapeDtypeStruct((half_e, vocab), F32),
                jax.ShapeDtypeStruct((layers, half_i, ff), F32),
                jax.ShapeDtypeStruct((layers, half_o, hid), F32),
            ],
            scratch_shapes=[
                pltpu.VMEM((2, stages, tokens, hid), BF16),
                pltpu.VMEM((2, stages, tokens, hid), F32),
                pltpu.VMEM((2, layers, half_i, ff), BF16),
                pltpu.VMEM((2, layers, half_o, hid), BF16),
                pltpu.VMEM((layers, half_i, ff), F32),
                pltpu.VMEM((layers, half_o, hid), F32),
                dma((7,)),
            ],
            compiler_params=pltpu.CompilerParams(vmem_limit_bytes=28 * 2**20),
        )(tok_ids, ids_peer, marks, resident(tab_own), resident(tab_peer), dx_all, gi_own, gi_recv, go_own, go_recv)
        return grad_in, grad_out, emb_t.T

    return jax.shard_map(device_body, mesh=mesh, in_specs=(P(None, 'dp'), P('pp', 'dp', None), P('pp', None, 'dp', None), P('pp', None, None), P('pp', None, None), P('pp', 'dp', None, None), P('pp', 'dp', None, None), P('dp', None, None)), out_specs=(P('pp', 'dp', None), P('pp', 'dp', None), P(None, 'dp')), check_vma=False)
```

```python
import functools

import jax
import jax.numpy as jnp
from jax import lax
from jax.experimental import pallas as pl
from jax.experimental.pallas import tpu as pltpu
from jax.sharding import PartitionSpec as P

MESH = pl.DeviceIdType.MESH
F32 = jnp.float32
BF16 = jnp.bfloat16
NT = (((1,), (1,)), ((), ()))
C0 = 0.7978845608028654
C1 = 0.7978845608028654 * 0.044715
FF_CHUNK = 256
GROUP = 32
BATCH = 2
LANES = 128
VOCAB_BLOCK = 5120
VOCAB_TILE = 256


def gelu_parts(pre_act):
    square = pre_act * pre_act
    tanh_val = jnp.tanh(pre_act * (C0 + C1 * square))
    half = 0.5 + 0.5 * tanh_val
    value = pre_act * half
    slope = half + (value - value * half) * (2.0 * C0 + (6.0 * C1) * square)
    return value, slope


def forward_layer(layer_id, w_in, w_out, acts_x, acts_a, acts_s):
    x_cur = acts_x[layer_id]
    out_x = x_cur.astype(F32)
    for start in range(0, w_in.shape[2], FF_CHUNK):
        cols = pl.ds(start, FF_CHUNK)
        pre_act = jnp.dot(x_cur, w_in[layer_id, :, cols], preferred_element_type=F32).astype(BF16)
        value, slope = gelu_parts(pre_act.astype(F32))
        hidden = value.astype(BF16)
        acts_a[layer_id, :, cols] = hidden
        acts_s[layer_id, :, cols] = slope
        out_x += jnp.dot(hidden, w_out[layer_id, cols, :], preferred_element_type=F32)
    acts_x[layer_id + 1] = out_x.astype(BF16)


def backward_layer(layer_id, w_in, w_out, acts_x, acts_a, acts_s, cot, sum_in, sum_out_t):
    cot_cur = cot[...]
    cot_t = cot_cur.T
    x_t = acts_x[layer_id].T
    d_x = cot_cur.astype(F32)
    for start in range(0, w_in.shape[2], FF_CHUNK):
        cols = pl.ds(start, FF_CHUNK)
        d_hidden = lax.dot_general(cot_cur, w_out[layer_id, cols, :], NT, preferred_element_type=F32).astype(BF16)
        d_pre = (d_hidden.astype(F32) * acts_s[layer_id, :, cols]).astype(BF16)
        d_x += lax.dot_general(d_pre, w_in[layer_id, :, cols], NT, preferred_element_type=F32)
        sum_out_t[layer_id, :, cols] += jnp.dot(cot_t, acts_a[layer_id, :, cols], preferred_element_type=F32)
        sum_in[layer_id, :, cols] += jnp.dot(x_t, d_pre, preferred_element_type=F32)
    cot[...] = d_x.astype(BF16)


def mark_repeats(ids):
    lane = lax.rem(lax.broadcasted_iota(jnp.int32, ids.shape, 1), GROUP)
    found = jnp.zeros_like(ids)
    for shift in range(1, GROUP):
        found = jnp.where((pltpu.roll(ids, shift, 1) == ids) & (lane >= shift), 1, found)
    shift = 1
    while shift < GROUP:
        found = found | pltpu.roll(found, ids.shape[1] - shift, 1)
        shift *= 2
    return found


def stage_kernel(stages, ids, d_out, stored_x, w_in, w_out, acc_in, acc_out, acc_emb,
                 marks, ids_own, ids_peer, tab_own, tab_peer, dx_all, gi_own, gi_recv, go_own, go_recv,
                 acts_x, acts_a, acts_s, cot, dx_send, cot_in, sum_in, sum_out_t, acc_o, mark_buf, ids_mine, ids_buf,
                 load_sem, ex_send, ex_recv, cot_send, cot_recv, bc_send, bc_recv, pr_send, pr_recv, loc_sem, g_sem, g_send, g_recv):
    stage = lax.axis_index('pp')
    rep = lax.axis_index('dp')
    other = 1 - rep
    layers = w_in.shape[0]
    last = stages - 1

    barrier = pltpu.get_barrier_semaphore()
    for hop in range(1, 2 * stages):
        place = lax.rem(stage * 2 + rep + hop, 2 * stages)
        pl.semaphore_signal(barrier, inc=1, device_id=(place // 2, lax.rem(place, 2)), device_id_type=MESH)

    load_in = pltpu.make_async_copy(acc_in, sum_in, load_sem.at[0])
    load_out = pltpu.make_async_copy(acc_out, acc_o, load_sem.at[1])
    load_in.start()
    load_out.start()
    vocab = acc_emb.shape[0]
    load_emb = pltpu.make_async_copy(acc_emb, tab_own.at[pl.ds(0, vocab)], load_sem.at[2])
    load_emb.start()
    sum_out_t[...] = jnp.zeros_like(sum_out_t)

    def forward(step_id):
        acts_x[0] = stored_x[last - stage - step_id]
        pl.loop(0, layers)(lambda layer_id: forward_layer(layer_id, w_in, w_out, acts_x, acts_a, acts_s))

    micros, tokens = ids.shape
    for block in range(tokens // LANES):
        ids_mine[pl.ds(block * micros, micros), :] = ids[:, pl.ds(block * LANES, LANES)]
    forward(0)
    pl.semaphore_wait(barrier, 2 * stages - 1)

    ex_ids = pltpu.make_async_remote_copy(ids_mine, ids_buf, ex_send.at[0], ex_recv.at[0], device_id=(stage, other), device_id_type=MESH)
    ex_emb = pltpu.make_async_remote_copy(acc_emb, tab_peer.at[pl.ds(0, vocab)], ex_send.at[1], ex_recv.at[1], device_id=(stage, other), device_id_type=MESH)
    ex_ids.start()
    ex_emb.start()
    load_in.wait()
    load_out.wait()

    def cot_copy(step_id):
        return pltpu.make_async_remote_copy(dx_send.at[step_id], cot_in.at[step_id], cot_send.at[step_id], cot_recv.at[step_id],
                                            device_id=(jnp.maximum(stage - 1, 0), rep), device_id_type=MESH)

    def bc_copy(step_id, target):
        return pltpu.make_async_remote_copy(dx_send.at[step_id], dx_all.at[rep, last - step_id], bc_send.at[target, step_id], bc_recv.at[step_id],
                                            device_id=(target, rep), device_id_type=MESH)

    def peer_copy(step_id, src):
        return pltpu.make_async_remote_copy(src, dx_all.at[rep, last - step_id], pr_send.at[step_id], pr_recv.at[step_id],
                                            device_id=(stage, other), device_id_type=MESH)

    def local_copy(step_id):
        return pltpu.make_async_copy(dx_send.at[step_id], dx_all.at[rep, last - step_id], loc_sem.at[step_id])

    @pl.loop(0, stages)
    def _(step_id):
        @pl.when(stage + step_id <= last)
        def _():
            @pl.when(step_id == 0)
            def _():
                cot[...] = d_out[...]

            @pl.when(step_id > 0)
            def _():
                forward(step_id)
                cot_copy(step_id - 1).wait_recv()
                cot[...] = cot_in[step_id - 1]

            pl.loop(0, layers)(lambda back_id: backward_layer(layers - 1 - back_id, w_in, w_out, acts_x, acts_a, acts_s, cot, sum_in, sum_out_t))
            dx_send[step_id] = cot[...]

            @pl.when(stage > 0)
            def _():
                cot_copy(step_id).start()

            @pl.when(stage == 0)
            def _():
                for target in range(1, stages):
                    bc_copy(step_id, target).start()
                peer_copy(step_id, dx_send.at[step_id]).start()
                local_copy(step_id).start()

    ex_ids.wait()
    mark_buf[...] = mark_repeats(ids_mine[...]) | mark_repeats(ids_buf[...])
    small = [
        pltpu.make_async_copy(mark_buf, marks, load_sem.at[3]),
        pltpu.make_async_copy(ids_buf, ids_peer, load_sem.at[4]),
        pltpu.make_async_copy(ids_mine, ids_own, load_sem.at[5]),
    ]
    for copy in small:
        copy.start()

    gi_bf = acts_a.at[:, pl.ds(0, w_in.shape[1]), :]
    go_bf = acts_x.at[pl.ds(0, layers)]

    @pl.loop(0, layers)
    def _(layer_id):
        gi_bf[layer_id] = sum_in[layer_id].astype(BF16)
        go_bf[layer_id] = (sum_out_t[layer_id].T + acc_o[layer_id]).astype(BF16)

    half_i = gi_own.shape[1]
    half_o = go_own.shape[1]
    keep = [
        pltpu.make_async_copy(gi_bf.at[:, pl.ds(pl.multiple_of(rep * half_i, half_i), half_i), :], gi_own, g_sem.at[0]),
        pltpu.make_async_copy(go_bf.at[:, pl.ds(pl.multiple_of(rep * half_o, half_o), half_o), :], go_own, g_sem.at[1]),
    ]
    give = [
        pltpu.make_async_remote_copy(gi_bf.at[:, pl.ds(pl.multiple_of(other * half_i, half_i), half_i), :], gi_recv, g_send.at[0], g_recv.at[0], device_id=(stage, other), device_id_type=MESH),
        pltpu.make_async_remote_copy(go_bf.at[:, pl.ds(pl.multiple_of(other * half_o, half_o), half_o), :], go_recv, g_send.at[1], g_recv.at[1], device_id=(stage, other), device_id_type=MESH),
    ]
    for copy in keep + give:
        copy.start()

    @pl.when(stage > 0)
    def _():
        for step_id in range(stages):
            bc_copy(step_id, 0).wait_recv()
            peer_copy(step_id, dx_all.at[rep, last - step_id]).start()
        for step_id in range(stages):
            @pl.when(stage + step_id <= last)
            def _():
                cot_copy(step_id).wait_send()

    @pl.when(stage == 0)
    def _():
        for step_id in range(stages):
            for target in range(1, stages):
                bc_copy(step_id, target).wait_send()
            local_copy(step_id).wait()

    for step_id in range(stages):
        peer_copy(step_id, dx_send.at[step_id]).wait()
    for copy in keep + give:
        copy.wait()
    for copy in small:
        copy.wait()
    ex_emb.wait()
    load_emb.wait()


def finish_kernel(ids_own, ids_peer, marks, tab_own, tab_peer, dx_all, gi_own, gi_recv, go_own, go_recv,
                  emb_t, grad_in, grad_out, dxf, gi_buf, go_buf, gi_out, go_out, sems):
    step = pl.program_id(0)
    rep = lax.axis_index('dp')
    padded = tab_own.shape[0]
    width = tab_own.shape[2]
    rows_own = tab_own.reshape(padded, width)
    rows_peer = tab_peer.reshape(padded, width)
    micros = dx_all.shape[1]
    loads = [pltpu.make_async_copy(src, dst, sems.at[pos]) for pos, (src, dst) in enumerate(
        ((gi_own, gi_buf.at[0]), (gi_recv, gi_buf.at[1]), (go_own, go_buf.at[0]), (go_recv, go_buf.at[1])))]
    stores = [pltpu.make_async_copy(gi_out, grad_in, sems.at[4]), pltpu.make_async_copy(go_out, grad_out, sems.at[5])]

    @pl.when(step == 0)
    def _():
        for copy in loads:
            copy.start()
        dxf[0] = dx_all[rep].astype(F32)
        dxf[1] = dx_all[1 - rep].astype(F32)
        sides = ((ids_own, rows_own, 0), (ids_peer, rows_peer, 1))

        @pl.loop(0, ids_own.shape[0])
        def _(line):
            micro = lax.rem(line, micros)
            token = (line // micros) * LANES

            @pl.loop(0, LANES // GROUP)
            def _(group):
                base = pl.multiple_of(group * GROUP, GROUP)
                repeated = marks[line, base] != 0

                @pl.when(repeated)
                def _():
                    @pl.loop(0, GROUP)
                    def _(pos):
                        for ids, rows, side in sides:
                            row = pl.ds(ids[line, base + pos], 1)
                            rows[row, :] = rows[row, :] + dxf[side, micro, pl.ds(token + base + pos, 1), :]

                @pl.when(jnp.logical_not(repeated))
                def _():
                    def add_batch(start):
                        sums = []
                        for ids, rows, side in sides:
                            for pos in range(start, start + BATCH):
                                row = pl.ds(ids[line, base + pos], 1)
                                sums.append((rows, row, rows[row, :] + dxf[side, micro, pl.ds(token + base + pos, 1), :]))
                        return sums

                    def store_batch(sums):
                        for rows, row, value in sums:
                            rows[row, :] = value

                    held = add_batch(0)
                    for start in range(BATCH, GROUP, BATCH):
                        fresh = add_batch(start)
                        store_batch(held)
                        held = fresh
                    store_batch(held)

        for copy in loads:
            copy.wait()
        gi_out[...] = (gi_buf[0].astype(F32) + gi_buf[1].astype(F32)) * 0.5
        go_out[...] = (go_buf[0].astype(F32) + go_buf[1].astype(F32)) * 0.5
        for copy in stores:
            copy.start()

    half = emb_t.shape[0]
    row_id = lax.broadcasted_iota(jnp.int32, (half, 2 * width), 0)
    col_id = lax.broadcasted_iota(jnp.int32, (half, 2 * width), 1)
    pick = jnp.where(lax.rem(col_id, width) == row_id + half * rep, 0.5, 0.0).astype(BF16)
    for start in range(0, emb_t.shape[1], VOCAB_TILE):
        first = pl.multiple_of(step * emb_t.shape[1] + start, 8)
        both = jnp.concatenate([rows_own[pl.ds(first, VOCAB_TILE), :].astype(BF16), rows_peer[pl.ds(first, VOCAB_TILE), :].astype(BF16)], axis=1)
        emb_t[:, start:start + VOCAB_TILE] = lax.dot_general(pick, both, NT, preferred_element_type=F32)

    @pl.when(step == pl.num_programs(0) - 1)
    def _():
        for copy in stores:
            copy.wait()


def solution(mesh):
    stages = mesh.shape['pp']

    def device_body(tok_ids, d_out, stored_x, w_in, w_out, acc_in, acc_out, acc_emb):
        layers, hid, ff = w_in.shape
        tokens = d_out.shape[1]
        vocab = acc_emb.shape[1]
        half_i, half_o, half_e = hid // 2, ff // 2, hid // 2
        emb_rows = acc_emb.reshape(vocab, 1, hid)
        lines = jax.ShapeDtypeStruct((tok_ids.size // LANES, LANES), tok_ids.dtype)
        table = pltpu.VMEM((pl.cdiv(vocab, VOCAB_BLOCK) * VOCAB_BLOCK, 1, hid), F32)
        any_spec = pl.BlockSpec(memory_space=pltpu.HBM)
        vmem_spec = pl.BlockSpec(memory_space=pltpu.VMEM)
        dma = pltpu.SemaphoreType.DMA
        marks, ids_own, ids_peer, tab_own, tab_peer, dx_all, gi_own, gi_recv, go_own, go_recv = pl.pallas_call(
            functools.partial(stage_kernel, stages),
            name='stage_pipeline',
            in_specs=[vmem_spec] * 5 + [any_spec] * 3,
            out_specs=[any_spec] * 3 + [vmem_spec] * 3 + [any_spec] * 4,
            out_shape=[
                lines,
                lines,
                lines,
                table,
                table,
                pltpu.VMEM((2, stages, tokens, hid), BF16),
                jax.ShapeDtypeStruct((layers, half_i, ff), BF16),
                jax.ShapeDtypeStruct((layers, half_i, ff), BF16),
                jax.ShapeDtypeStruct((layers, half_o, hid), BF16),
                jax.ShapeDtypeStruct((layers, half_o, hid), BF16),
            ],
            scratch_shapes=[
                pltpu.VMEM((layers + 1, tokens, hid), BF16),
                pltpu.VMEM((layers, tokens, ff), BF16),
                pltpu.VMEM((layers, tokens, ff), F32),
                pltpu.VMEM((tokens, hid), BF16),
                pltpu.VMEM((stages, tokens, hid), BF16),
                pltpu.VMEM((stages, tokens, hid), BF16),
                pltpu.VMEM((layers, hid, ff), F32),
                pltpu.VMEM((layers, hid, ff), F32),
                pltpu.VMEM((layers, ff, hid), F32),
                pltpu.VMEM(lines.shape, jnp.int32),
                pltpu.VMEM(lines.shape, jnp.int32),
                pltpu.VMEM(lines.shape, jnp.int32),
                dma((6,)), dma((2,)), dma((2,)),
                dma((stages,)), dma((stages,)),
                dma((stages, stages)), dma((stages,)),
                dma((stages,)), dma((stages,)), dma((stages,)),
                dma((2,)), dma((2,)), dma((2,)),
            ],
            compiler_params=pltpu.CompilerParams(collective_id=0, has_side_effects=True, vmem_limit_bytes=28 * 2**20),
        )(tok_ids, d_out[0], stored_x[0], w_in, w_out, acc_in[:, 0], acc_out[:, 0], emb_rows)

        resident = lambda x: pltpu.with_memory_space_constraint(x, pltpu.VMEM)
        smem_spec = pl.BlockSpec(memory_space=pltpu.SMEM)
        emb_t, grad_in, grad_out = pl.pallas_call(
            finish_kernel,
            name='finish',
            grid=(pl.cdiv(vocab, VOCAB_BLOCK),),
            in_specs=[smem_spec] * 3 + [vmem_spec] * 3 + [any_spec] * 4,
            out_specs=[pl.BlockSpec((half_e, VOCAB_BLOCK), lambda step: (0, step))] + [any_spec] * 2,
            out_shape=[
                jax.ShapeDtypeStruct((half_e, vocab), F32),
                jax.ShapeDtypeStruct((layers, half_i, ff), F32),
                jax.ShapeDtypeStruct((layers, half_o, hid), F32),
            ],
            scratch_shapes=[
                pltpu.VMEM((2, stages, tokens, hid), F32),
                pltpu.VMEM((2, layers, half_i, ff), BF16),
                pltpu.VMEM((2, layers, half_o, hid), BF16),
                pltpu.VMEM((layers, half_i, ff), F32),
                pltpu.VMEM((layers, half_o, hid), F32),
                dma((6,)),
            ],
            compiler_params=pltpu.CompilerParams(vmem_limit_bytes=28 * 2**20),
        )(ids_own, ids_peer, marks, resident(tab_own), resident(tab_peer), resident(dx_all), gi_own, gi_recv, go_own, go_recv)
        return grad_in, grad_out, emb_t.T

    return jax.shard_map(device_body, mesh=mesh, in_specs=(P(None, 'dp'), P('pp', 'dp', None), P('pp', None, 'dp', None), P('pp', None, None), P('pp', None, None), P('pp', 'dp', None, None), P('pp', 'dp', None, None), P('dp', None, None)), out_specs=(P('pp', 'dp', None), P('pp', 'dp', None), P(None, 'dp')), check_vma=False)
```

```python
import functools

import jax
import jax.numpy as jnp
from jax import lax
from jax.experimental import pallas as pl
from jax.experimental.pallas import tpu as pltpu
from jax.sharding import PartitionSpec as P

MESH = pl.DeviceIdType.MESH
F32 = jnp.float32
BF16 = jnp.bfloat16
NT = (((1,), (1,)), ((), ()))
C0 = 0.7978845608028654
C1 = 0.7978845608028654 * 0.044715
FF_CHUNK = 256
STRIDE = 8
PARTS = 2
GROUP = 32
BATCH = 2
LANES = 128
VOCAB_BLOCK = 5120
VOCAB_TILE = 256


def gelu_parts(pre_act):
    square = pre_act * pre_act
    tanh_val = jnp.tanh(pre_act * (C0 + C1 * square))
    half = 0.5 + 0.5 * tanh_val
    value = pre_act * half
    slope = half + (value - value * half) * (2.0 * C0 + (6.0 * C1) * square)
    return value, slope


def forward_layer(layer_id, rows, w_in, w_out, acts_x, acts_a, acts_s):
    x_cur = acts_x[layer_id, rows, :]
    out_x = x_cur.astype(F32)
    for start in range(0, w_in.shape[2], FF_CHUNK):
        cols = pl.ds(start, FF_CHUNK)
        pre_act = jnp.dot(x_cur, w_in[layer_id, :, cols], preferred_element_type=F32).astype(BF16)
        value, slope = gelu_parts(pre_act.astype(F32))
        hidden = value.astype(BF16)
        acts_a[layer_id, rows, cols] = hidden
        acts_s[layer_id, rows, cols] = slope
        out_x += jnp.dot(hidden, w_out[layer_id, cols, :], preferred_element_type=F32)
    acts_x[layer_id + 1, rows, :] = out_x.astype(BF16)


def backward_layer(layer_id, rows, w_in, w_out, acts_x, acts_a, acts_s, cot, sum_in, sum_out_t):
    cot_cur = cot[rows, :]
    d_x = cot_cur.astype(F32)
    d_pres = []
    for start in range(0, w_in.shape[2], FF_CHUNK):
        cols = pl.ds(start, FF_CHUNK)
        d_hidden = lax.dot_general(cot_cur, w_out[layer_id, cols, :], NT, preferred_element_type=F32).astype(BF16)
        d_pre = (d_hidden.astype(F32) * acts_s[layer_id, rows, cols]).astype(BF16)
        d_pres.append(d_pre)
        d_x += lax.dot_general(d_pre, w_in[layer_id, :, cols], NT, preferred_element_type=F32)
    cot[rows, :] = d_x.astype(BF16)
    cot_t = cot_cur.T
    x_t = acts_x[layer_id, rows, :].T
    for start, d_pre in zip(range(0, w_in.shape[2], FF_CHUNK), d_pres):
        cols = pl.ds(start, FF_CHUNK)
        sum_out_t[layer_id, :, cols] += jnp.dot(cot_t, acts_a[layer_id, rows, cols], preferred_element_type=F32)
        sum_in[layer_id, :, cols] += jnp.dot(x_t, d_pre, preferred_element_type=F32)


def each_layer(layers, tokens, step):
    part = tokens // PARTS

    @pl.loop(0, layers // STRIDE)
    def _(turn):
        for pos in range(STRIDE):
            for index in range(PARTS):
                step(turn * STRIDE + pos, pl.ds(index * part, part))


def mark_repeats(ids):
    lane = lax.rem(lax.broadcasted_iota(jnp.int32, ids.shape, 1), GROUP)
    found = jnp.zeros_like(ids)
    for shift in range(1, GROUP):
        found = jnp.where((pltpu.roll(ids, shift, 1) == ids) & (lane >= shift), 1, found)
    shift = 1
    while shift < GROUP:
        found = found | pltpu.roll(found, ids.shape[1] - shift, 1)
        shift *= 2
    return found


def stage_kernel(stages, ids, d_out, stored_x, w_in, w_out, acc_in, acc_out, acc_emb,
                 marks, ids_own, ids_peer, tab_own, tab_peer, dx_all, gi_own, gi_recv, go_own, go_recv,
                 acts_x, acts_a, acts_s, cot, dx_send, cot_in, sum_in, sum_out_t, acc_o, mark_buf, ids_mine, ids_buf,
                 load_sem, ex_send, ex_recv, cot_send, cot_recv, bc_send, bc_recv, pr_send, pr_recv, loc_sem, g_sem, g_send, g_recv):
    stage = lax.axis_index('pp')
    rep = lax.axis_index('dp')
    other = 1 - rep
    layers = w_in.shape[0]
    last = stages - 1

    barrier = pltpu.get_barrier_semaphore()
    for hop in range(1, 2 * stages):
        place = lax.rem(stage * 2 + rep + hop, 2 * stages)
        pl.semaphore_signal(barrier, inc=1, device_id=(place // 2, lax.rem(place, 2)), device_id_type=MESH)

    load_in = pltpu.make_async_copy(acc_in, sum_in, load_sem.at[0])
    load_out = pltpu.make_async_copy(acc_out, acc_o, load_sem.at[1])
    load_in.start()
    load_out.start()
    vocab = acc_emb.shape[0]
    load_emb = pltpu.make_async_copy(acc_emb, tab_own.at[pl.ds(0, vocab)], load_sem.at[2])
    load_emb.start()
    sum_out_t[...] = jnp.zeros_like(sum_out_t)

    def forward(step_id):
        acts_x[0] = stored_x[last - stage - step_id]
        each_layer(layers, tokens, lambda layer_id, rows: forward_layer(layer_id, rows, w_in, w_out, acts_x, acts_a, acts_s))

    micros, tokens = ids.shape
    for block in range(tokens // LANES):
        ids_mine[pl.ds(block * micros, micros), :] = ids[:, pl.ds(block * LANES, LANES)]
    ex_ids = pltpu.make_async_remote_copy(ids_mine, ids_buf, ex_send.at[0], ex_recv.at[0], device_id=(stage, other), device_id_type=MESH)
    ex_emb = pltpu.make_async_remote_copy(acc_emb, tab_peer.at[pl.ds(0, vocab)], ex_send.at[1], ex_recv.at[1], device_id=(stage, other), device_id_type=MESH)

    def cot_copy(step_id):
        return pltpu.make_async_remote_copy(dx_send.at[step_id], cot_in.at[step_id], cot_send.at[step_id], cot_recv.at[step_id],
                                            device_id=(jnp.maximum(stage - 1, 0), rep), device_id_type=MESH)

    def bc_copy(step_id, target):
        return pltpu.make_async_remote_copy(dx_send.at[step_id], dx_all.at[rep, last - step_id], bc_send.at[target, step_id], bc_recv.at[step_id],
                                            device_id=(target, rep), device_id_type=MESH)

    def peer_copy(step_id, src):
        return pltpu.make_async_remote_copy(src, dx_all.at[rep, last - step_id], pr_send.at[step_id], pr_recv.at[step_id],
                                            device_id=(stage, other), device_id_type=MESH)

    def local_copy(step_id):
        return pltpu.make_async_copy(dx_send.at[step_id], dx_all.at[rep, last - step_id], loc_sem.at[step_id])

    @pl.loop(0, stages)
    def _(step_id):
        @pl.when(stage + step_id <= last)
        def _():
            forward(step_id)

            @pl.when(step_id == 0)
            def _():
                pl.semaphore_wait(barrier, 2 * stages - 1)
                ex_ids.start()
                ex_emb.start()
                load_in.wait()
                load_out.wait()
                cot[...] = d_out[...]

            @pl.when(step_id > 0)
            def _():
                cot_copy(step_id - 1).wait_recv()
                cot[...] = cot_in[step_id - 1]

            each_layer(layers, tokens, lambda back_id, rows: backward_layer(layers - 1 - back_id, rows, w_in, w_out, acts_x, acts_a, acts_s, cot, sum_in, sum_out_t))
            dx_send[step_id] = cot[...]

            @pl.when(stage > 0)
            def _():
                cot_copy(step_id).start()

            @pl.when(stage == 0)
            def _():
                for target in range(1, stages):
                    bc_copy(step_id, target).start()
                peer_copy(step_id, dx_send.at[step_id]).start()
                local_copy(step_id).start()

    ex_ids.wait()
    mark_buf[...] = mark_repeats(ids_mine[...]) | mark_repeats(ids_buf[...])
    small = [
        pltpu.make_async_copy(mark_buf, marks, load_sem.at[3]),
        pltpu.make_async_copy(ids_buf, ids_peer, load_sem.at[4]),
        pltpu.make_async_copy(ids_mine, ids_own, load_sem.at[5]),
    ]
    for copy in small:
        copy.start()

    gi_bf = acts_a.at[:, pl.ds(0, w_in.shape[1]), :]
    go_bf = acts_x.at[pl.ds(0, layers)]

    @pl.loop(0, layers)
    def _(layer_id):
        gi_bf[layer_id] = sum_in[layer_id].astype(BF16)
        go_bf[layer_id] = (sum_out_t[layer_id].T + acc_o[layer_id]).astype(BF16)

    half_i = gi_own.shape[1]
    half_o = go_own.shape[1]
    keep = [
        pltpu.make_async_copy(gi_bf.at[:, pl.ds(pl.multiple_of(rep * half_i, half_i), half_i), :], gi_own, g_sem.at[0]),
        pltpu.make_async_copy(go_bf.at[:, pl.ds(pl.multiple_of(rep * half_o, half_o), half_o), :], go_own, g_sem.at[1]),
    ]
    give = [
        pltpu.make_async_remote_copy(gi_bf.at[:, pl.ds(pl.multiple_of(other * half_i, half_i), half_i), :], gi_recv, g_send.at[0], g_recv.at[0], device_id=(stage, other), device_id_type=MESH),
        pltpu.make_async_remote_copy(go_bf.at[:, pl.ds(pl.multiple_of(other * half_o, half_o), half_o), :], go_recv, g_send.at[1], g_recv.at[1], device_id=(stage, other), device_id_type=MESH),
    ]
    for copy in keep + give:
        copy.start()

    @pl.when(stage > 0)
    def _():
        for step_id in range(stages):
            bc_copy(step_id, 0).wait_recv()
            peer_copy(step_id, dx_all.at[rep, last - step_id]).start()
        for step_id in range(stages):
            @pl.when(stage + step_id <= last)
            def _():
                cot_copy(step_id).wait_send()

    @pl.when(stage == 0)
    def _():
        for step_id in range(stages):
            for target in range(1, stages):
                bc_copy(step_id, target).wait_send()
            local_copy(step_id).wait()

    for step_id in range(stages):
        peer_copy(step_id, dx_send.at[step_id]).wait()
    for copy in keep + give:
        copy.wait()
    for copy in small:
        copy.wait()
    ex_emb.wait()
    load_emb.wait()


def finish_kernel(ids_own, ids_peer, marks, tab_own, tab_peer, dx_all, gi_own, gi_recv, go_own, go_recv,
                  emb_t, grad_in, grad_out, dxf, gi_buf, go_buf, gi_out, go_out, sems):
    step = pl.program_id(0)
    rep = lax.axis_index('dp')
    padded = tab_own.shape[0]
    width = tab_own.shape[2]
    rows_own = tab_own.reshape(padded, width)
    rows_peer = tab_peer.reshape(padded, width)
    micros = dx_all.shape[1]
    loads = [pltpu.make_async_copy(src, dst, sems.at[pos]) for pos, (src, dst) in enumerate(
        ((gi_own, gi_buf.at[0]), (gi_recv, gi_buf.at[1]), (go_own, go_buf.at[0]), (go_recv, go_buf.at[1])))]
    stores = [pltpu.make_async_copy(gi_out, grad_in, sems.at[4]), pltpu.make_async_copy(go_out, grad_out, sems.at[5])]

    @pl.when(step == 0)
    def _():
        for copy in loads:
            copy.start()
        dxf[0] = dx_all[rep].astype(F32)
        dxf[1] = dx_all[1 - rep].astype(F32)
        sides = ((ids_own, rows_own, 0), (ids_peer, rows_peer, 1))

        @pl.loop(0, ids_own.shape[0])
        def _(line):
            micro = lax.rem(line, micros)
            token = (line // micros) * LANES

            @pl.loop(0, LANES // GROUP)
            def _(group):
                base = pl.multiple_of(group * GROUP, GROUP)
                repeated = marks[line, base] != 0

                @pl.when(repeated)
                def _():
                    @pl.loop(0, GROUP)
                    def _(pos):
                        for ids, rows, side in sides:
                            row = pl.ds(ids[line, base + pos], 1)
                            rows[row, :] = rows[row, :] + dxf[side, micro, pl.ds(token + base + pos, 1), :]

                @pl.when(jnp.logical_not(repeated))
                def _():
                    def add_batch(start):
                        sums = []
                        for ids, rows, side in sides:
                            for pos in range(start, start + BATCH):
                                row = pl.ds(ids[line, base + pos], 1)
                                sums.append((rows, row, rows[row, :] + dxf[side, micro, pl.ds(token + base + pos, 1), :]))
                        return sums

                    def store_batch(sums):
                        for rows, row, value in sums:
                            rows[row, :] = value

                    held = add_batch(0)
                    for start in range(BATCH, GROUP, BATCH):
                        fresh = add_batch(start)
                        store_batch(held)
                        held = fresh
                    store_batch(held)

        for copy in loads:
            copy.wait()
        gi_out[...] = (gi_buf[0].astype(F32) + gi_buf[1].astype(F32)) * 0.5
        go_out[...] = (go_buf[0].astype(F32) + go_buf[1].astype(F32)) * 0.5
        for copy in stores:
            copy.start()

    half = emb_t.shape[0]
    row_id = lax.broadcasted_iota(jnp.int32, (half, 2 * width), 0)
    col_id = lax.broadcasted_iota(jnp.int32, (half, 2 * width), 1)
    pick = jnp.where(lax.rem(col_id, width) == row_id + half * rep, 0.5, 0.0).astype(BF16)
    for start in range(0, emb_t.shape[1], VOCAB_TILE):
        first = pl.multiple_of(step * emb_t.shape[1] + start, 8)
        both = jnp.concatenate([rows_own[pl.ds(first, VOCAB_TILE), :].astype(BF16), rows_peer[pl.ds(first, VOCAB_TILE), :].astype(BF16)], axis=1)
        emb_t[:, start:start + VOCAB_TILE] = lax.dot_general(pick, both, NT, preferred_element_type=F32)

    @pl.when(step == pl.num_programs(0) - 1)
    def _():
        for copy in stores:
            copy.wait()


def solution(mesh):
    stages = mesh.shape['pp']

    def device_body(tok_ids, d_out, stored_x, w_in, w_out, acc_in, acc_out, acc_emb):
        layers, hid, ff = w_in.shape
        tokens = d_out.shape[1]
        vocab = acc_emb.shape[1]
        half_i, half_o, half_e = hid // 2, ff // 2, hid // 2
        emb_rows = acc_emb.reshape(vocab, 1, hid)
        lines = jax.ShapeDtypeStruct((tok_ids.size // LANES, LANES), tok_ids.dtype)
        table = pltpu.VMEM((pl.cdiv(vocab, VOCAB_BLOCK) * VOCAB_BLOCK, 1, hid), F32)
        any_spec = pl.BlockSpec(memory_space=pltpu.HBM)
        vmem_spec = pl.BlockSpec(memory_space=pltpu.VMEM)
        dma = pltpu.SemaphoreType.DMA
        marks, ids_own, ids_peer, tab_own, tab_peer, dx_all, gi_own, gi_recv, go_own, go_recv = pl.pallas_call(
            functools.partial(stage_kernel, stages),
            name='stage_pipeline',
            in_specs=[vmem_spec] * 5 + [any_spec] * 3,
            out_specs=[any_spec] * 3 + [vmem_spec] * 3 + [any_spec] * 4,
            out_shape=[
                lines,
                lines,
                lines,
                table,
                table,
                pltpu.VMEM((2, stages, tokens, hid), BF16),
                jax.ShapeDtypeStruct((layers, half_i, ff), BF16),
                jax.ShapeDtypeStruct((layers, half_i, ff), BF16),
                jax.ShapeDtypeStruct((layers, half_o, hid), BF16),
                jax.ShapeDtypeStruct((layers, half_o, hid), BF16),
            ],
            scratch_shapes=[
                pltpu.VMEM((layers + 1, tokens, hid), BF16),
                pltpu.VMEM((layers, tokens, ff), BF16),
                pltpu.VMEM((layers, tokens, ff), F32),
                pltpu.VMEM((tokens, hid), BF16),
                pltpu.VMEM((stages, tokens, hid), BF16),
                pltpu.VMEM((stages, tokens, hid), BF16),
                pltpu.VMEM((layers, hid, ff), F32),
                pltpu.VMEM((layers, hid, ff), F32),
                pltpu.VMEM((layers, ff, hid), F32),
                pltpu.VMEM(lines.shape, jnp.int32),
                pltpu.VMEM(lines.shape, jnp.int32),
                pltpu.VMEM(lines.shape, jnp.int32),
                dma((6,)), dma((2,)), dma((2,)),
                dma((stages,)), dma((stages,)),
                dma((stages, stages)), dma((stages,)),
                dma((stages,)), dma((stages,)), dma((stages,)),
                dma((2,)), dma((2,)), dma((2,)),
            ],
            compiler_params=pltpu.CompilerParams(collective_id=0, has_side_effects=True, vmem_limit_bytes=28 * 2**20),
        )(tok_ids, d_out[0], stored_x[0], w_in, w_out, acc_in[:, 0], acc_out[:, 0], emb_rows)

        resident = lambda x: pltpu.with_memory_space_constraint(x, pltpu.VMEM)
        smem_spec = pl.BlockSpec(memory_space=pltpu.SMEM)
        emb_t, grad_in, grad_out = pl.pallas_call(
            finish_kernel,
            name='finish',
            grid=(pl.cdiv(vocab, VOCAB_BLOCK),),
            in_specs=[smem_spec] * 3 + [vmem_spec] * 3 + [any_spec] * 4,
            out_specs=[pl.BlockSpec((half_e, VOCAB_BLOCK), lambda step: (0, step))] + [any_spec] * 2,
            out_shape=[
                jax.ShapeDtypeStruct((half_e, vocab), F32),
                jax.ShapeDtypeStruct((layers, half_i, ff), F32),
                jax.ShapeDtypeStruct((layers, half_o, hid), F32),
            ],
            scratch_shapes=[
                pltpu.VMEM((2, stages, tokens, hid), F32),
                pltpu.VMEM((2, layers, half_i, ff), BF16),
                pltpu.VMEM((2, layers, half_o, hid), BF16),
                pltpu.VMEM((layers, half_i, ff), F32),
                pltpu.VMEM((layers, half_o, hid), F32),
                dma((6,)),
            ],
            compiler_params=pltpu.CompilerParams(vmem_limit_bytes=28 * 2**20),
        )(ids_own, ids_peer, marks, resident(tab_own), resident(tab_peer), resident(dx_all), gi_own, gi_recv, go_own, go_recv)
        return grad_in, grad_out, emb_t.T

    return jax.shard_map(device_body, mesh=mesh, in_specs=(P(None, 'dp'), P('pp', 'dp', None), P('pp', None, 'dp', None), P('pp', None, None), P('pp', None, None), P('pp', 'dp', None, None), P('pp', 'dp', None, None), P('dp', None, None)), out_specs=(P('pp', 'dp', None), P('pp', 'dp', None), P(None, 'dp')), check_vma=False)
```

```python
import functools

import jax
import jax.numpy as jnp
from jax import lax
from jax.experimental import pallas as pl
from jax.experimental.pallas import tpu as pltpu
from jax.sharding import PartitionSpec as P

MESH = pl.DeviceIdType.MESH
F32 = jnp.float32
BF16 = jnp.bfloat16
NT = (((1,), (1,)), ((), ()))
C0 = 0.7978845608028654
C1 = 0.7978845608028654 * 0.044715
FF_CHUNK = 256
FORWARD_PARTS = 2
BACKWARD_PARTS = 1
GROUP = 32
BATCH = 2
LANES = 128
CHUNKS = 4
ROUTES = {1: (0, 1, 2, 3), 2: (2, 3, 0, 1), 3: (0, 2, 1, 3)}
VOCAB_BLOCK = 5120
VOCAB_TILE = 256


def gelu_parts(half_act):
    cubic = (8.0 * C1) * (half_act * half_act)
    tanh_val = jnp.tanh(half_act * (2.0 * C0 + cubic))
    upper = 1.0 + tanh_val
    value = half_act * upper
    slope = upper + (value * (1.0 - tanh_val)) * (2.0 * C0 + 3.0 * cubic)
    return value, slope


def forward_layer(layer_id, rows, final, w_half, w_out, acts_x, acts_a, acts_s):
    x_cur = acts_x[layer_id, rows, :]
    out_x = x_cur.astype(F32)
    for start in range(0, w_half.shape[2], FF_CHUNK):
        cols = pl.ds(start, FF_CHUNK)
        half_act = jnp.dot(x_cur, w_half[layer_id, :, cols], preferred_element_type=F32).astype(BF16)
        value, slope = gelu_parts(half_act.astype(F32))
        hidden = value.astype(BF16)
        acts_a[layer_id, rows, cols] = hidden
        acts_s[layer_id, rows, cols] = slope
        if not final:
            out_x += jnp.dot(hidden, w_out[layer_id, cols, :], preferred_element_type=F32)
    if not final:
        acts_x[layer_id + 1, rows, :] = out_x.astype(BF16)


def backward_layer(layer_id, rows, w_half, w_out, acts_x, acts_a, acts_s, cot, sum_in, sum_out_t):
    cot_cur = cot[rows, :]
    d_x = cot_cur.astype(F32)
    d_pres = []
    for start in range(0, w_half.shape[2], FF_CHUNK):
        cols = pl.ds(start, FF_CHUNK)
        d_hidden = lax.dot_general(cot_cur, w_out[layer_id, cols, :], NT, preferred_element_type=F32).astype(BF16)
        d_pre = (d_hidden.astype(F32) * acts_s[layer_id, rows, cols]).astype(BF16)
        d_pres.append(d_pre)
        d_x += lax.dot_general(d_pre, w_half[layer_id, :, cols], NT, preferred_element_type=F32)
    cot[rows, :] = d_x.astype(BF16)
    cot_t = cot_cur.T
    x_t = (acts_x[layer_id, rows, :].astype(F32) * 0.5).astype(BF16).T
    for start, d_pre in zip(range(0, w_half.shape[2], FF_CHUNK), d_pres):
        cols = pl.ds(start, FF_CHUNK)
        sum_out_t[layer_id, :, cols] += jnp.dot(cot_t, acts_a[layer_id, rows, cols], preferred_element_type=F32)
        sum_in[layer_id, :, cols] += jnp.dot(x_t, d_pre, preferred_element_type=F32)


def each_layer(layers, tokens, parts, step):
    part = tokens // parts
    for layer_id in range(layers):
        for index in range(parts):
            step(layer_id, pl.ds(index * part, part))


def mark_repeats(ids):
    lane = lax.rem(lax.broadcasted_iota(jnp.int32, ids.shape, 1), GROUP)
    found = jnp.zeros_like(ids)
    for shift in range(1, GROUP):
        found = jnp.where((pltpu.roll(ids, shift, 1) == ids) & (lane >= shift), 1, found)
    shift = 1
    while shift < GROUP:
        found = found | pltpu.roll(found, ids.shape[1] - shift, 1)
        shift *= 2
    return found


def stage_kernel(stages, ids, d_out, stored_x, w_in, w_out, acc_in, acc_out, acc_emb,
                 marks, ids_own, ids_peer, tab_own, tab_peer, dx_all, gi_own, gi_recv, go_own, go_recv,
                 w_half, acts_x, acts_a, acts_s, cot, dx_send, cot_in, sum_in, sum_out_t, acc_o, mark_buf, ids_mine, ids_buf,
                 load_sem, ex_send, ex_recv, cot_send, cot_recv, bc_send, bc_recv, pr_send, pr_recv, loc_sem, g_sem, g_send, g_recv):
    stage = lax.axis_index('pp')
    rep = lax.axis_index('dp')
    other = 1 - rep
    layers = w_in.shape[0]
    last = stages - 1

    barrier = pltpu.get_barrier_semaphore()
    for hop in range(1, 2 * stages):
        place = lax.rem(stage * 2 + rep + hop, 2 * stages)
        pl.semaphore_signal(barrier, inc=1, device_id=(place // 2, lax.rem(place, 2)), device_id_type=MESH)

    load_in = pltpu.make_async_copy(acc_in, sum_in, load_sem.at[0])
    load_out = pltpu.make_async_copy(acc_out, acc_o, load_sem.at[1])
    load_in.start()
    load_out.start()
    vocab = acc_emb.shape[0]
    load_emb = pltpu.make_async_copy(acc_emb, tab_own.at[pl.ds(0, vocab)], load_sem.at[2])
    load_emb.start()
    sum_out_t[...] = jnp.zeros_like(sum_out_t)
    w_half[...] = (w_in[...].astype(F32) * 0.5).astype(BF16)

    def forward(step_id):
        acts_x[0] = stored_x[last - stage - step_id]
        each_layer(layers, tokens, FORWARD_PARTS, lambda layer_id, rows: forward_layer(layer_id, rows, layer_id == layers - 1, w_half, w_out, acts_x, acts_a, acts_s))

    micros, tokens = ids.shape
    for block in range(tokens // LANES):
        ids_mine[pl.ds(block * micros, micros), :] = ids[:, pl.ds(block * LANES, LANES)]
    ex_ids = pltpu.make_async_remote_copy(ids_mine, ids_buf, ex_send.at[0], ex_recv.at[0], device_id=(stage, other), device_id_type=MESH)
    ex_emb = pltpu.make_async_remote_copy(acc_emb, tab_peer.at[pl.ds(0, vocab)], ex_send.at[1], ex_recv.at[1], device_id=(stage, other), device_id_type=MESH)

    def cot_copy(step_id):
        return pltpu.make_async_remote_copy(dx_send.at[step_id], cot_in.at[step_id], cot_send.at[step_id], cot_recv.at[step_id],
                                            device_id=(jnp.maximum(stage - 1, 0), rep), device_id_type=MESH)

    chunk_rows = d_out.shape[0] // CHUNKS

    def piece(step_id, chunk):
        return dx_all.at[rep, last - step_id, pl.ds(chunk * chunk_rows, chunk_rows)]

    def sent(step_id, chunk):
        return dx_send.at[step_id, pl.ds(chunk * chunk_rows, chunk_rows)]

    def bc_copy(step_id, chunk, target):
        return pltpu.make_async_remote_copy(sent(step_id, chunk), piece(step_id, chunk), bc_send.at[target, step_id, chunk], bc_recv.at[step_id, chunk],
                                            device_id=(target, rep), device_id_type=MESH)

    def relay_copy(step_id, chunk):
        return pltpu.make_async_remote_copy(piece(step_id, chunk), piece(step_id, chunk), bc_send.at[last, step_id, chunk], bc_recv.at[step_id, chunk],
                                            device_id=(last, rep), device_id_type=MESH)

    def peer_copy(step_id, chunk, src):
        return pltpu.make_async_remote_copy(src, piece(step_id, chunk), pr_send.at[step_id, chunk], pr_recv.at[step_id, chunk],
                                            device_id=(stage, other), device_id_type=MESH)

    def local_copy(step_id):
        return pltpu.make_async_copy(dx_send.at[step_id], dx_all.at[rep, last - step_id], loc_sem.at[step_id])

    @pl.loop(0, stages)
    def _(step_id):
        @pl.when(stage + step_id <= last)
        def _():
            forward(step_id)

            @pl.when(step_id == 0)
            def _():
                pl.semaphore_wait(barrier, 2 * stages - 1)
                ex_ids.start()
                ex_emb.start()
                load_in.wait()
                load_out.wait()
                cot[...] = d_out[...]

            @pl.when(step_id > 0)
            def _():
                cot_copy(step_id - 1).wait_recv()
                cot[...] = cot_in[step_id - 1]

            each_layer(layers, tokens, BACKWARD_PARTS, lambda back_id, rows: backward_layer(layers - 1 - back_id, rows, w_half, w_out, acts_x, acts_a, acts_s, cot, sum_in, sum_out_t))
            dx_send[step_id] = cot[...]

            @pl.when(stage > 0)
            def _():
                cot_copy(step_id).start()

            @pl.when(stage == 0)
            def _():
                for first, second in zip(ROUTES[1], ROUTES[2]):
                    bc_copy(step_id, first, 1).start()
                    bc_copy(step_id, second, 2).start()
                for chunk in range(CHUNKS):
                    peer_copy(step_id, chunk, sent(step_id, chunk)).start()
                local_copy(step_id).start()

    ex_ids.wait()
    mark_buf[...] = mark_repeats(ids_mine[...]) | mark_repeats(ids_buf[...])
    small = [
        pltpu.make_async_copy(mark_buf, marks, load_sem.at[3]),
        pltpu.make_async_copy(ids_buf, ids_peer, load_sem.at[4]),
        pltpu.make_async_copy(ids_mine, ids_own, load_sem.at[5]),
    ]
    for copy in small:
        copy.start()

    gi_bf = acts_a.at[:, pl.ds(0, w_in.shape[1]), :]
    go_bf = acts_x.at[pl.ds(0, layers)]

    @pl.loop(0, layers)
    def _(layer_id):
        gi_bf[layer_id] = sum_in[layer_id].astype(BF16)
        go_bf[layer_id] = (sum_out_t[layer_id].T + acc_o[layer_id]).astype(BF16)

    half_i = gi_own.shape[1]
    half_o = go_own.shape[1]
    keep = [
        pltpu.make_async_copy(gi_bf.at[:, pl.ds(pl.multiple_of(rep * half_i, half_i), half_i), :], gi_own, g_sem.at[0]),
        pltpu.make_async_copy(go_bf.at[:, pl.ds(pl.multiple_of(rep * half_o, half_o), half_o), :], go_own, g_sem.at[1]),
    ]
    give = [
        pltpu.make_async_remote_copy(gi_bf.at[:, pl.ds(pl.multiple_of(other * half_i, half_i), half_i), :], gi_recv, g_send.at[0], g_recv.at[0], device_id=(stage, other), device_id_type=MESH),
        pltpu.make_async_remote_copy(go_bf.at[:, pl.ds(pl.multiple_of(other * half_o, half_o), half_o), :], go_recv, g_send.at[1], g_recv.at[1], device_id=(stage, other), device_id_type=MESH),
    ]
    for copy in keep + give:
        copy.start()

    for place, order in ROUTES.items():
        @pl.when(stage == place)
        def _():
            for step_id in range(stages):
                for pos, chunk in enumerate(order):
                    bc_copy(step_id, chunk, 0).wait_recv()
                    if place < last and pos < CHUNKS // 2:
                        relay_copy(step_id, chunk).start()
                    peer_copy(step_id, chunk, piece(step_id, chunk)).start()
            for step_id in range(stages):
                if place < last:
                    for chunk in order[:CHUNKS // 2]:
                        relay_copy(step_id, chunk).wait_send()
                if place + step_id <= last:
                    cot_copy(step_id).wait_send()

    @pl.when(stage == 0)
    def _():
        for step_id in range(stages):
            for chunk in range(CHUNKS):
                for target in (1, 2):
                    bc_copy(step_id, chunk, target).wait_send()
            local_copy(step_id).wait()

    for step_id in range(stages):
        for chunk in range(CHUNKS):
            peer_copy(step_id, chunk, sent(step_id, chunk)).wait()
    for copy in keep + give:
        copy.wait()
    for copy in small:
        copy.wait()
    ex_emb.wait()
    load_emb.wait()


def finish_kernel(ids_own, ids_peer, marks, tab_own, tab_peer, dx_all, gi_own, gi_recv, go_own, go_recv,
                  emb_t, grad_in, grad_out, dxf, gi_buf, go_buf, gi_out, go_out, sems):
    step = pl.program_id(0)
    rep = lax.axis_index('dp')
    padded = tab_own.shape[0]
    width = tab_own.shape[2]
    rows_own = tab_own.reshape(padded, width)
    rows_peer = tab_peer.reshape(padded, width)
    micros = dx_all.shape[1]
    loads = [pltpu.make_async_copy(src, dst, sems.at[pos]) for pos, (src, dst) in enumerate(
        ((gi_own, gi_buf.at[0]), (gi_recv, gi_buf.at[1]), (go_own, go_buf.at[0]), (go_recv, go_buf.at[1])))]
    stores = [pltpu.make_async_copy(gi_out, grad_in, sems.at[4]), pltpu.make_async_copy(go_out, grad_out, sems.at[5])]

    @pl.when(step == 0)
    def _():
        for copy in loads:
            copy.start()
        dxf[0] = dx_all[rep].astype(F32)
        dxf[1] = dx_all[1 - rep].astype(F32)
        sides = ((ids_own, rows_own, 0), (ids_peer, rows_peer, 1))

        @pl.loop(0, ids_own.shape[0])
        def _(line):
            micro = lax.rem(line, micros)
            token = (line // micros) * LANES

            @pl.loop(0, LANES // GROUP)
            def _(group):
                base = pl.multiple_of(group * GROUP, GROUP)
                repeated = marks[line, base] != 0

                @pl.when(repeated)
                def _():
                    @pl.loop(0, GROUP)
                    def _(pos):
                        for ids, rows, side in sides:
                            row = pl.ds(ids[line, base + pos], 1)
                            rows[row, :] = rows[row, :] + dxf[side, micro, pl.ds(token + base + pos, 1), :]

                @pl.when(jnp.logical_not(repeated))
                def _():
                    def add_batch(start):
                        sums = []
                        for ids, rows, side in sides:
                            for pos in range(start, start + BATCH):
                                row = pl.ds(ids[line, base + pos], 1)
                                sums.append((rows, row, rows[row, :] + dxf[side, micro, pl.ds(token + base + pos, 1), :]))
                        return sums

                    def store_batch(sums):
                        for rows, row, value in sums:
                            rows[row, :] = value

                    held = add_batch(0)
                    for start in range(BATCH, GROUP, BATCH):
                        fresh = add_batch(start)
                        store_batch(held)
                        held = fresh
                    store_batch(held)

        for copy in loads:
            copy.wait()
        gi_out[...] = (gi_buf[0].astype(F32) + gi_buf[1].astype(F32)) * 0.5
        go_out[...] = (go_buf[0].astype(F32) + go_buf[1].astype(F32)) * 0.5
        for copy in stores:
            copy.start()

    half = emb_t.shape[0]
    row_id = lax.broadcasted_iota(jnp.int32, (half, width), 0)
    col_id = lax.broadcasted_iota(jnp.int32, (half, width), 1)
    pick = jnp.where(lax.rem(col_id, half) == row_id, 0.5, 0.0).astype(BF16)
    mine = lax.broadcasted_iota(jnp.int32, (VOCAB_TILE, width), 1) // half == rep
    for start in range(0, emb_t.shape[1], VOCAB_TILE):
        rows = pl.ds(pl.multiple_of(step * emb_t.shape[1] + start, 8), VOCAB_TILE)
        both = jnp.where(mine, rows_own[rows, :], pltpu.roll(rows_peer[rows, :], half, 1)).astype(BF16)
        emb_t[:, start:start + VOCAB_TILE] = lax.dot_general(pick, both, NT, preferred_element_type=F32)

    @pl.when(step == pl.num_programs(0) - 1)
    def _():
        for copy in stores:
            copy.wait()


def solution(mesh):
    stages = mesh.shape['pp']

    def device_body(tok_ids, d_out, stored_x, w_in, w_out, acc_in, acc_out, acc_emb):
        layers, hid, ff = w_in.shape
        tokens = d_out.shape[1]
        vocab = acc_emb.shape[1]
        half_i, half_o, half_e = hid // 2, ff // 2, hid // 2
        emb_rows = acc_emb.reshape(vocab, 1, hid)
        lines = jax.ShapeDtypeStruct((tok_ids.size // LANES, LANES), tok_ids.dtype)
        table = pltpu.VMEM((pl.cdiv(vocab, VOCAB_BLOCK) * VOCAB_BLOCK, 1, hid), F32)
        any_spec = pl.BlockSpec(memory_space=pltpu.HBM)
        vmem_spec = pl.BlockSpec(memory_space=pltpu.VMEM)
        dma = pltpu.SemaphoreType.DMA
        marks, ids_own, ids_peer, tab_own, tab_peer, dx_all, gi_own, gi_recv, go_own, go_recv = pl.pallas_call(
            functools.partial(stage_kernel, stages),
            name='stage_pipeline',
            in_specs=[vmem_spec] * 5 + [any_spec] * 3,
            out_specs=[any_spec] * 3 + [vmem_spec] * 3 + [any_spec] * 4,
            out_shape=[
                lines,
                lines,
                lines,
                table,
                table,
                pltpu.VMEM((2, stages, tokens, hid), BF16),
                jax.ShapeDtypeStruct((layers, half_i, ff), BF16),
                jax.ShapeDtypeStruct((layers, half_i, ff), BF16),
                jax.ShapeDtypeStruct((layers, half_o, hid), BF16),
                jax.ShapeDtypeStruct((layers, half_o, hid), BF16),
            ],
            scratch_shapes=[
                pltpu.VMEM((layers, hid, ff), BF16),
                pltpu.VMEM((layers + 1, tokens, hid), BF16),
                pltpu.VMEM((layers, tokens, ff), BF16),
                pltpu.VMEM((layers, tokens, ff), F32),
                pltpu.VMEM((tokens, hid), BF16),
                pltpu.VMEM((stages, tokens, hid), BF16),
                pltpu.VMEM((stages, tokens, hid), BF16),
                pltpu.VMEM((layers, hid, ff), F32),
                pltpu.VMEM((layers, hid, ff), F32),
                pltpu.VMEM((layers, ff, hid), F32),
                pltpu.VMEM(lines.shape, jnp.int32),
                pltpu.VMEM(lines.shape, jnp.int32),
                pltpu.VMEM(lines.shape, jnp.int32),
                dma((6,)), dma((2,)), dma((2,)),
                dma((stages,)), dma((stages,)),
                dma((stages, stages, CHUNKS)), dma((stages, CHUNKS)),
                dma((stages, CHUNKS)), dma((stages, CHUNKS)), dma((stages,)),
                dma((2,)), dma((2,)), dma((2,)),
            ],
            compiler_params=pltpu.CompilerParams(collective_id=0, has_side_effects=True, vmem_limit_bytes=30 * 2**20),
        )(tok_ids, d_out[0], stored_x[0], w_in, w_out, acc_in[:, 0], acc_out[:, 0], emb_rows)

        resident = lambda x: pltpu.with_memory_space_constraint(x, pltpu.VMEM)
        smem_spec = pl.BlockSpec(memory_space=pltpu.SMEM)
        emb_t, grad_in, grad_out = pl.pallas_call(
            finish_kernel,
            name='finish',
            grid=(pl.cdiv(vocab, VOCAB_BLOCK),),
            in_specs=[smem_spec] * 3 + [vmem_spec] * 3 + [any_spec] * 4,
            out_specs=[pl.BlockSpec((half_e, VOCAB_BLOCK), lambda step: (0, step))] + [any_spec] * 2,
            out_shape=[
                jax.ShapeDtypeStruct((half_e, vocab), F32),
                jax.ShapeDtypeStruct((layers, half_i, ff), F32),
                jax.ShapeDtypeStruct((layers, half_o, hid), F32),
            ],
            scratch_shapes=[
                pltpu.VMEM((2, stages, tokens, hid), F32),
                pltpu.VMEM((2, layers, half_i, ff), BF16),
                pltpu.VMEM((2, layers, half_o, hid), BF16),
                pltpu.VMEM((layers, half_i, ff), F32),
                pltpu.VMEM((layers, half_o, hid), F32),
                dma((6,)),
            ],
            compiler_params=pltpu.CompilerParams(vmem_limit_bytes=30 * 2**20),
        )(ids_own, ids_peer, marks, resident(tab_own), resident(tab_peer), resident(dx_all), gi_own, gi_recv, go_own, go_recv)
        return grad_in, grad_out, emb_t.T

    return jax.shard_map(device_body, mesh=mesh, in_specs=(P(None, 'dp'), P('pp', 'dp', None), P('pp', None, 'dp', None), P('pp', None, None), P('pp', None, None), P('pp', 'dp', None, None), P('pp', 'dp', None, None), P('dp', None, None)), out_specs=(P('pp', 'dp', None), P('pp', 'dp', None), P(None, 'dp')), check_vma=False)
```

```python
import functools

import jax
import jax.numpy as jnp
from jax import lax
from jax.experimental import pallas as pl
from jax.experimental.pallas import tpu as pltpu
from jax.sharding import PartitionSpec as P

MESH = pl.DeviceIdType.MESH
F32 = jnp.float32
BF16 = jnp.bfloat16
NT = (((1,), (1,)), ((), ()))
C0 = 0.7978845608028654
C1 = 0.7978845608028654 * 0.044715
FF_CHUNK = 256
FORWARD_PARTS = 2
BACKWARD_PARTS = 1
GROUP = 32
BATCH = 4
LANES = 128
CHUNKS = 4
ROUTES = {1: (0, 1, 2, 3), 2: (2, 3, 0, 1), 3: (0, 2, 1, 3)}
VOCAB_BLOCK = 5120
VOCAB_TILE = 256


def gelu_parts(half_act):
    cubic = (8.0 * C1) * (half_act * half_act)
    tanh_val = jnp.tanh(half_act * (2.0 * C0 + cubic))
    upper = 1.0 + tanh_val
    value = half_act * upper
    slope = upper + (value * (1.0 - tanh_val)) * (2.0 * C0 + 3.0 * cubic)
    return value, slope


def forward_layer(layer_id, rows, final, w_half, w_out, acts_x, acts_a, acts_s):
    x_cur = acts_x[layer_id, rows, :]
    out_x = x_cur.astype(F32)
    for start in range(0, w_half.shape[2], FF_CHUNK):
        cols = pl.ds(start, FF_CHUNK)
        half_act = jnp.dot(x_cur, w_half[layer_id, :, cols], preferred_element_type=F32).astype(BF16)
        value, slope = gelu_parts(half_act.astype(F32))
        hidden = value.astype(BF16)
        acts_a[layer_id, rows, cols] = hidden
        acts_s[layer_id, rows, cols] = slope
        if not final:
            out_x += jnp.dot(hidden, w_out[layer_id, cols, :], preferred_element_type=F32)
    if not final:
        acts_x[layer_id + 1, rows, :] = out_x.astype(BF16)


def backward_layer(layer_id, rows, w_half, w_out, acts_x, acts_a, acts_s, cot, sum_in, sum_out_t):
    cot_cur = cot[rows, :]
    d_x = cot_cur.astype(F32)
    d_pres = []
    for start in range(0, w_half.shape[2], FF_CHUNK):
        cols = pl.ds(start, FF_CHUNK)
        d_hidden = lax.dot_general(cot_cur, w_out[layer_id, cols, :], NT, preferred_element_type=F32).astype(BF16)
        d_pre = (d_hidden.astype(F32) * acts_s[layer_id, rows, cols]).astype(BF16)
        d_pres.append(d_pre)
        d_x += lax.dot_general(d_pre, w_half[layer_id, :, cols], NT, preferred_element_type=F32)
    cot[rows, :] = d_x.astype(BF16)
    cot_t = cot_cur.T
    x_t = (acts_x[layer_id, rows, :].astype(F32) * 0.5).astype(BF16).T
    for start, d_pre in zip(range(0, w_half.shape[2], FF_CHUNK), d_pres):
        cols = pl.ds(start, FF_CHUNK)
        sum_out_t[layer_id, :, cols] += jnp.dot(cot_t, acts_a[layer_id, rows, cols], preferred_element_type=F32)
        sum_in[layer_id, :, cols] += jnp.dot(x_t, d_pre, preferred_element_type=F32)


def each_layer(layers, tokens, parts, step):
    part = tokens // parts
    for layer_id in range(layers):
        for index in range(parts):
            step(layer_id, pl.ds(index * part, part))


def mark_repeats(ids):
    lane = lax.rem(lax.broadcasted_iota(jnp.int32, ids.shape, 1), GROUP)
    found = jnp.zeros_like(ids)
    for shift in range(1, GROUP):
        found = jnp.where((pltpu.roll(ids, shift, 1) == ids) & (lane >= shift), 1, found)
    shift = 1
    while shift < GROUP:
        found = found | pltpu.roll(found, ids.shape[1] - shift, 1)
        shift *= 2
    return found


def stage_kernel(stages, ids, d_out, stored_x, w_in, w_out, acc_in, acc_out, acc_emb,
                 marks, ids_own, ids_peer, tab_own, tab_peer, dx_all, gi_own, gi_recv, go_own, go_recv,
                 w_half, acts_x, acts_a, acts_s, cot, dx_send, cot_in, sum_in, sum_out_t, acc_o, mark_buf, ids_mine, ids_buf,
                 load_sem, ex_send, ex_recv, cot_send, cot_recv, bc_send, bc_recv, pr_send, pr_recv, loc_sem, g_sem, g_send, g_recv):
    stage = lax.axis_index('pp')
    rep = lax.axis_index('dp')
    other = 1 - rep
    layers = w_in.shape[0]
    last = stages - 1

    barrier = pltpu.get_barrier_semaphore()
    for hop in range(1, 2 * stages):
        place = lax.rem(stage * 2 + rep + hop, 2 * stages)
        pl.semaphore_signal(barrier, inc=1, device_id=(place // 2, lax.rem(place, 2)), device_id_type=MESH)

    load_in = pltpu.make_async_copy(acc_in, sum_in, load_sem.at[0])
    load_out = pltpu.make_async_copy(acc_out, acc_o, load_sem.at[1])
    load_in.start()
    load_out.start()
    vocab = acc_emb.shape[0]
    load_emb = pltpu.make_async_copy(acc_emb, tab_own.at[pl.ds(0, vocab)], load_sem.at[2])
    load_emb.start()
    sum_out_t[...] = jnp.zeros_like(sum_out_t)
    w_half[...] = (w_in[...].astype(F32) * 0.5).astype(BF16)

    def forward(step_id):
        acts_x[0] = stored_x[last - stage - step_id]
        each_layer(layers, tokens, FORWARD_PARTS, lambda layer_id, rows: forward_layer(layer_id, rows, layer_id == layers - 1, w_half, w_out, acts_x, acts_a, acts_s))

    micros, tokens = ids.shape
    for block in range(tokens // LANES):
        ids_mine[pl.ds(block * micros, micros), :] = ids[:, pl.ds(block * LANES, LANES)]
    ex_ids = pltpu.make_async_remote_copy(ids_mine, ids_buf, ex_send.at[0], ex_recv.at[0], device_id=(stage, other), device_id_type=MESH)
    ex_emb = pltpu.make_async_remote_copy(acc_emb, tab_peer.at[pl.ds(0, vocab)], ex_send.at[1], ex_recv.at[1], device_id=(stage, other), device_id_type=MESH)

    def cot_copy(step_id):
        return pltpu.make_async_remote_copy(dx_send.at[step_id], cot_in.at[step_id], cot_send.at[step_id], cot_recv.at[step_id],
                                            device_id=(jnp.maximum(stage - 1, 0), rep), device_id_type=MESH)

    chunk_rows = d_out.shape[0] // CHUNKS

    def piece(step_id, chunk):
        return dx_all.at[rep, last - step_id, pl.ds(chunk * chunk_rows, chunk_rows)]

    def sent(step_id, chunk):
        return dx_send.at[step_id, pl.ds(chunk * chunk_rows, chunk_rows)]

    def bc_copy(step_id, chunk, target):
        return pltpu.make_async_remote_copy(sent(step_id, chunk), piece(step_id, chunk), bc_send.at[target, step_id, chunk], bc_recv.at[step_id, chunk],
                                            device_id=(target, rep), device_id_type=MESH)

    def relay_copy(step_id, chunk):
        return pltpu.make_async_remote_copy(piece(step_id, chunk), piece(step_id, chunk), bc_send.at[last, step_id, chunk], bc_recv.at[step_id, chunk],
                                            device_id=(last, rep), device_id_type=MESH)

    def peer_copy(step_id, chunk, src):
        return pltpu.make_async_remote_copy(src, piece(step_id, chunk), pr_send.at[step_id, chunk], pr_recv.at[step_id, chunk],
                                            device_id=(stage, other), device_id_type=MESH)

    def local_copy(step_id):
        return pltpu.make_async_copy(dx_send.at[step_id], dx_all.at[rep, last - step_id], loc_sem.at[step_id])

    @pl.loop(0, stages)
    def _(step_id):
        @pl.when(stage + step_id <= last)
        def _():
            forward(step_id)

            @pl.when(step_id == 0)
            def _():
                pl.semaphore_wait(barrier, 2 * stages - 1)
                ex_ids.start()
                ex_emb.start()
                load_in.wait()
                load_out.wait()
                cot[...] = d_out[...]

            @pl.when(step_id > 0)
            def _():
                cot_copy(step_id - 1).wait_recv()
                cot[...] = cot_in[step_id - 1]

            each_layer(layers, tokens, BACKWARD_PARTS, lambda back_id, rows: backward_layer(layers - 1 - back_id, rows, w_half, w_out, acts_x, acts_a, acts_s, cot, sum_in, sum_out_t))
            dx_send[step_id] = cot[...]

            @pl.when(stage > 0)
            def _():
                cot_copy(step_id).start()

            @pl.when(stage == 0)
            def _():
                for first, second in zip(ROUTES[1], ROUTES[2]):
                    bc_copy(step_id, first, 1).start()
                    bc_copy(step_id, second, 2).start()
                for chunk in range(CHUNKS):
                    peer_copy(step_id, chunk, sent(step_id, chunk)).start()
                local_copy(step_id).start()

    ex_ids.wait()
    mark_buf[...] = mark_repeats(ids_mine[...]) | mark_repeats(ids_buf[...])
    small = [
        pltpu.make_async_copy(mark_buf, marks, load_sem.at[3]),
        pltpu.make_async_copy(ids_buf, ids_peer, load_sem.at[4]),
        pltpu.make_async_copy(ids_mine, ids_own, load_sem.at[5]),
    ]
    for copy in small:
        copy.start()

    gi_bf = acts_a.at[:, pl.ds(0, w_in.shape[1]), :]
    go_bf = acts_x.at[pl.ds(0, layers)]

    @pl.loop(0, layers)
    def _(layer_id):
        gi_bf[layer_id] = sum_in[layer_id].astype(BF16)
        go_bf[layer_id] = (sum_out_t[layer_id].T + acc_o[layer_id]).astype(BF16)

    half_i = gi_own.shape[1]
    half_o = go_own.shape[1]
    keep = [
        pltpu.make_async_copy(gi_bf.at[:, pl.ds(pl.multiple_of(rep * half_i, half_i), half_i), :], gi_own, g_sem.at[0]),
        pltpu.make_async_copy(go_bf.at[:, pl.ds(pl.multiple_of(rep * half_o, half_o), half_o), :], go_own, g_sem.at[1]),
    ]
    give = [
        pltpu.make_async_remote_copy(gi_bf.at[:, pl.ds(pl.multiple_of(other * half_i, half_i), half_i), :], gi_recv, g_send.at[0], g_recv.at[0], device_id=(stage, other), device_id_type=MESH),
        pltpu.make_async_remote_copy(go_bf.at[:, pl.ds(pl.multiple_of(other * half_o, half_o), half_o), :], go_recv, g_send.at[1], g_recv.at[1], device_id=(stage, other), device_id_type=MESH),
    ]
    for copy in keep + give:
        copy.start()

    for place, order in ROUTES.items():
        @pl.when(stage == place)
        def _():
            for step_id in range(stages):
                for pos, chunk in enumerate(order):
                    bc_copy(step_id, chunk, 0).wait_recv()
                    if place < last and pos < CHUNKS // 2:
                        relay_copy(step_id, chunk).start()
                    peer_copy(step_id, chunk, piece(step_id, chunk)).start()
            for step_id in range(stages):
                if place < last:
                    for chunk in order[:CHUNKS // 2]:
                        relay_copy(step_id, chunk).wait_send()
                if place + step_id <= last:
                    cot_copy(step_id).wait_send()

    @pl.when(stage == 0)
    def _():
        for step_id in range(stages):
            for chunk in range(CHUNKS):
                for target in (1, 2):
                    bc_copy(step_id, chunk, target).wait_send()
            local_copy(step_id).wait()

    for step_id in range(stages):
        for chunk in range(CHUNKS):
            peer_copy(step_id, chunk, sent(step_id, chunk)).wait()
    for copy in keep + give:
        copy.wait()
    for copy in small:
        copy.wait()
    ex_emb.wait()
    load_emb.wait()


def finish_kernel(ids_own, ids_peer, marks, tab_own, tab_peer, dx_all, gi_own, gi_recv, go_own, go_recv,
                  emb_t, grad_in, grad_out, dxf, gi_buf, go_buf, gi_out, go_out, sems):
    step = pl.program_id(0)
    rep = lax.axis_index('dp')
    padded = tab_own.shape[0]
    width = tab_own.shape[2]
    rows_own = tab_own.reshape(padded, width)
    rows_peer = tab_peer.reshape(padded, width)
    micros = dx_all.shape[1]
    loads = [pltpu.make_async_copy(src, dst, sems.at[pos]) for pos, (src, dst) in enumerate(
        ((gi_own, gi_buf.at[0]), (gi_recv, gi_buf.at[1]), (go_own, go_buf.at[0]), (go_recv, go_buf.at[1])))]
    stores = [pltpu.make_async_copy(gi_out, grad_in, sems.at[4]), pltpu.make_async_copy(go_out, grad_out, sems.at[5])]

    @pl.when(step == 0)
    def _():
        for copy in loads:
            copy.start()
        dxf[0] = dx_all[rep].astype(F32)
        dxf[1] = dx_all[1 - rep].astype(F32)
        sides = ((ids_own, rows_own, 0), (ids_peer, rows_peer, 1))

        @pl.loop(0, ids_own.shape[0])
        def _(line):
            micro = lax.rem(line, micros)
            token = (line // micros) * LANES

            for base in range(0, LANES, GROUP):
                repeated = marks[line, base] != 0

                @pl.when(repeated)
                def _():
                    @pl.loop(0, GROUP)
                    def _(pos):
                        for ids, rows, side in sides:
                            row = pl.ds(ids[line, base + pos], 1)
                            rows[row, :] = rows[row, :] + dxf[side, micro, pl.ds(token + base + pos, 1), :]

                @pl.when(jnp.logical_not(repeated))
                def _():
                    def add_batch(start):
                        sums = []
                        for ids, rows, side in sides:
                            for pos in range(start, start + BATCH):
                                row = pl.ds(ids[line, base + pos], 1)
                                sums.append((rows, row, rows[row, :] + dxf[side, micro, pl.ds(token + base + pos, 1), :]))
                        return sums

                    def store_batch(sums):
                        for rows, row, value in sums:
                            rows[row, :] = value

                    held = add_batch(0)
                    for start in range(BATCH, GROUP, BATCH):
                        fresh = add_batch(start)
                        store_batch(held)
                        held = fresh
                    store_batch(held)

        for copy in loads:
            copy.wait()
        gi_out[...] = (gi_buf[0].astype(F32) + gi_buf[1].astype(F32)) * 0.5
        go_out[...] = (go_buf[0].astype(F32) + go_buf[1].astype(F32)) * 0.5
        for copy in stores:
            copy.start()

    half = emb_t.shape[0]
    row_id = lax.broadcasted_iota(jnp.int32, (half, width), 0)
    col_id = lax.broadcasted_iota(jnp.int32, (half, width), 1)
    pick = jnp.where(lax.rem(col_id, half) == row_id, 0.5, 0.0).astype(BF16)
    mine = lax.broadcasted_iota(jnp.int32, (VOCAB_TILE, width), 1) // half == rep
    for start in range(0, emb_t.shape[1], VOCAB_TILE):
        rows = pl.ds(pl.multiple_of(step * emb_t.shape[1] + start, 8), VOCAB_TILE)
        both = jnp.where(mine, rows_own[rows, :], pltpu.roll(rows_peer[rows, :], half, 1)).astype(BF16)
        emb_t[:, start:start + VOCAB_TILE] = lax.dot_general(pick, both, NT, preferred_element_type=F32)

    @pl.when(step == pl.num_programs(0) - 1)
    def _():
        for copy in stores:
            copy.wait()


def solution(mesh):
    stages = mesh.shape['pp']

    def device_body(tok_ids, d_out, stored_x, w_in, w_out, acc_in, acc_out, acc_emb):
        layers, hid, ff = w_in.shape
        tokens = d_out.shape[1]
        vocab = acc_emb.shape[1]
        half_i, half_o, half_e = hid // 2, ff // 2, hid // 2
        emb_rows = acc_emb.reshape(vocab, 1, hid)
        lines = jax.ShapeDtypeStruct((tok_ids.size // LANES, LANES), tok_ids.dtype)
        table = pltpu.VMEM((pl.cdiv(vocab, VOCAB_BLOCK) * VOCAB_BLOCK, 1, hid), F32)
        any_spec = pl.BlockSpec(memory_space=pltpu.HBM)
        vmem_spec = pl.BlockSpec(memory_space=pltpu.VMEM)
        dma = pltpu.SemaphoreType.DMA
        marks, ids_own, ids_peer, tab_own, tab_peer, dx_all, gi_own, gi_recv, go_own, go_recv = pl.pallas_call(
            functools.partial(stage_kernel, stages),
            name='stage_pipeline',
            in_specs=[vmem_spec] * 5 + [any_spec] * 3,
            out_specs=[any_spec] * 3 + [vmem_spec] * 3 + [any_spec] * 4,
            out_shape=[
                lines,
                lines,
                lines,
                table,
                table,
                pltpu.VMEM((2, stages, tokens, hid), BF16),
                jax.ShapeDtypeStruct((layers, half_i, ff), BF16),
                jax.ShapeDtypeStruct((layers, half_i, ff), BF16),
                jax.ShapeDtypeStruct((layers, half_o, hid), BF16),
                jax.ShapeDtypeStruct((layers, half_o, hid), BF16),
            ],
            scratch_shapes=[
                pltpu.VMEM((layers, hid, ff), BF16),
                pltpu.VMEM((layers + 1, tokens, hid), BF16),
                pltpu.VMEM((layers, tokens, ff), BF16),
                pltpu.VMEM((layers, tokens, ff), F32),
                pltpu.VMEM((tokens, hid), BF16),
                pltpu.VMEM((stages, tokens, hid), BF16),
                pltpu.VMEM((stages, tokens, hid), BF16),
                pltpu.VMEM((layers, hid, ff), F32),
                pltpu.VMEM((layers, hid, ff), F32),
                pltpu.VMEM((layers, ff, hid), F32),
                pltpu.VMEM(lines.shape, jnp.int32),
                pltpu.VMEM(lines.shape, jnp.int32),
                pltpu.VMEM(lines.shape, jnp.int32),
                dma((6,)), dma((2,)), dma((2,)),
                dma((stages,)), dma((stages,)),
                dma((stages, stages, CHUNKS)), dma((stages, CHUNKS)),
                dma((stages, CHUNKS)), dma((stages, CHUNKS)), dma((stages,)),
                dma((2,)), dma((2,)), dma((2,)),
            ],
            compiler_params=pltpu.CompilerParams(collective_id=0, has_side_effects=True, vmem_limit_bytes=30 * 2**20),
        )(tok_ids, d_out[0], stored_x[0], w_in, w_out, acc_in[:, 0], acc_out[:, 0], emb_rows)

        resident = lambda x: pltpu.with_memory_space_constraint(x, pltpu.VMEM)
        smem_spec = pl.BlockSpec(memory_space=pltpu.SMEM)
        emb_t, grad_in, grad_out = pl.pallas_call(
            finish_kernel,
            name='finish',
            grid=(pl.cdiv(vocab, VOCAB_BLOCK),),
            in_specs=[smem_spec] * 3 + [vmem_spec] * 3 + [any_spec] * 4,
            out_specs=[pl.BlockSpec((half_e, VOCAB_BLOCK), lambda step: (0, step))] + [any_spec] * 2,
            out_shape=[
                jax.ShapeDtypeStruct((half_e, vocab), F32),
                jax.ShapeDtypeStruct((layers, half_i, ff), F32),
                jax.ShapeDtypeStruct((layers, half_o, hid), F32),
            ],
            scratch_shapes=[
                pltpu.VMEM((2, stages, tokens, hid), F32),
                pltpu.VMEM((2, layers, half_i, ff), BF16),
                pltpu.VMEM((2, layers, half_o, hid), BF16),
                pltpu.VMEM((layers, half_i, ff), F32),
                pltpu.VMEM((layers, half_o, hid), F32),
                dma((6,)),
            ],
            compiler_params=pltpu.CompilerParams(vmem_limit_bytes=30 * 2**20),
        )(ids_own, ids_peer, marks, resident(tab_own), resident(tab_peer), resident(dx_all), gi_own, gi_recv, go_own, go_recv)
        return grad_in, grad_out, emb_t.T

    return jax.shard_map(device_body, mesh=mesh, in_specs=(P(None, 'dp'), P('pp', 'dp', None), P('pp', None, 'dp', None), P('pp', None, None), P('pp', None, None), P('pp', 'dp', None, None), P('pp', 'dp', None, None), P('dp', None, None)), out_specs=(P('pp', 'dp', None), P('pp', 'dp', None), P(None, 'dp')), check_vma=False)
```

```python
import functools

import jax
import jax.numpy as jnp
from jax import lax
from jax.experimental import pallas as pl
from jax.experimental.pallas import tpu as pltpu
from jax.sharding import PartitionSpec as P

MESH = pl.DeviceIdType.MESH
F32 = jnp.float32
BF16 = jnp.bfloat16
NT = (((1,), (1,)), ((), ()))
C0 = 0.7978845608028654
C1 = 0.7978845608028654 * 0.044715
FF_CHUNK = 256
FORWARD_PARTS = 2
BACKWARD_PARTS = 1
GROUP = 32
BATCH = 4
LANES = 128
CHUNKS = 4
ROUTES = {1: (0, 1, 2, 3), 2: (2, 3, 0, 1), 3: (0, 2, 1, 3)}
VOCAB_BLOCK = 7680
VOCAB_TILE = 256


def gelu_parts(half_act):
    cubic = (8.0 * C1) * (half_act * half_act)
    tanh_val = jnp.tanh(half_act * (2.0 * C0 + cubic))
    upper = 1.0 + tanh_val
    value = half_act * upper
    slope = upper + (value * (1.0 - tanh_val)) * (2.0 * C0 + 3.0 * cubic)
    return value, slope


def forward_layer(layer_id, rows, final, w_half, w_out, acts_x, acts_a, acts_s):
    x_cur = acts_x[layer_id, rows, :]
    out_x = x_cur.astype(F32)
    for start in range(0, w_half.shape[2], FF_CHUNK):
        cols = pl.ds(start, FF_CHUNK)
        half_act = jnp.dot(x_cur, w_half[layer_id, :, cols], preferred_element_type=F32).astype(BF16)
        value, slope = gelu_parts(half_act.astype(F32))
        hidden = value.astype(BF16)
        acts_a[layer_id, rows, cols] = hidden
        acts_s[layer_id, rows, cols] = slope
        if not final:
            out_x += jnp.dot(hidden, w_out[layer_id, cols, :], preferred_element_type=F32)
    if not final:
        acts_x[layer_id + 1, rows, :] = out_x.astype(BF16)


def backward_layer(layer_id, rows, w_half, w_out, acts_x, acts_a, acts_s, cot, sum_in, sum_out_t):
    cot_cur = cot[rows, :]
    d_x = cot_cur.astype(F32)
    d_pres = []
    for start in range(0, w_half.shape[2], FF_CHUNK):
        cols = pl.ds(start, FF_CHUNK)
        d_hidden = lax.dot_general(cot_cur, w_out[layer_id, cols, :], NT, preferred_element_type=F32).astype(BF16)
        d_pre = (d_hidden.astype(F32) * acts_s[layer_id, rows, cols]).astype(BF16)
        d_pres.append(d_pre)
        d_x += lax.dot_general(d_pre, w_half[layer_id, :, cols], NT, preferred_element_type=F32)
    cot[rows, :] = d_x.astype(BF16)
    cot_t = cot_cur.T
    x_t = (acts_x[layer_id, rows, :].astype(F32) * 0.5).astype(BF16).T
    for start, d_pre in zip(range(0, w_half.shape[2], FF_CHUNK), d_pres):
        cols = pl.ds(start, FF_CHUNK)
        sum_out_t[layer_id, :, cols] += jnp.dot(cot_t, acts_a[layer_id, rows, cols], preferred_element_type=F32)
        sum_in[layer_id, :, cols] += jnp.dot(x_t, d_pre, preferred_element_type=F32)


def each_layer(layers, tokens, parts, step):
    part = tokens // parts
    for layer_id in range(layers):
        for index in range(parts):
            step(layer_id, pl.ds(index * part, part))


def mark_repeats(ids):
    lane = lax.rem(lax.broadcasted_iota(jnp.int32, ids.shape, 1), GROUP)
    found = jnp.zeros_like(ids)
    for shift in range(1, GROUP):
        found = jnp.where((pltpu.roll(ids, shift, 1) == ids) & (lane >= shift), 1, found)
    shift = 1
    while shift < GROUP:
        found = found | pltpu.roll(found, ids.shape[1] - shift, 1)
        shift *= 2
    return found


def stage_kernel(stages, ids, d_out, stored_x, w_in, w_out, acc_in, acc_out, acc_emb,
                 marks, ids_own, ids_peer, tab_own, tab_peer, dx_all, gi_own, gi_recv, go_own, go_recv,
                 w_half, acts_x, acts_a, acts_s, cot, dx_send, cot_in, sum_in, sum_out_t, acc_o, mark_buf, ids_mine, ids_buf,
                 load_sem, ex_send, ex_recv, cot_send, cot_recv, bc_send, bc_recv, pr_send, pr_recv, loc_sem, g_sem, g_send, g_recv):
    stage = lax.axis_index('pp')
    rep = lax.axis_index('dp')
    other = 1 - rep
    layers = w_in.shape[0]
    last = stages - 1

    barrier = pltpu.get_barrier_semaphore()
    for hop in range(1, 2 * stages):
        place = lax.rem(stage * 2 + rep + hop, 2 * stages)
        pl.semaphore_signal(barrier, inc=1, device_id=(place // 2, lax.rem(place, 2)), device_id_type=MESH)

    load_in = pltpu.make_async_copy(acc_in, sum_in, load_sem.at[0])
    load_out = pltpu.make_async_copy(acc_out, acc_o, load_sem.at[1])
    load_in.start()
    load_out.start()
    vocab = acc_emb.shape[0]
    load_emb = pltpu.make_async_copy(acc_emb, tab_own.at[pl.ds(0, vocab)], load_sem.at[2])
    load_emb.start()
    sum_out_t[...] = jnp.zeros_like(sum_out_t)
    w_half[...] = (w_in[...].astype(F32) * 0.5).astype(BF16)

    def forward(step_id):
        acts_x[0] = stored_x[last - stage - step_id]
        each_layer(layers, tokens, FORWARD_PARTS, lambda layer_id, rows: forward_layer(layer_id, rows, layer_id == layers - 1, w_half, w_out, acts_x, acts_a, acts_s))

    micros, tokens = ids.shape
    for block in range(tokens // LANES):
        ids_mine[pl.ds(block * micros, micros), :] = ids[:, pl.ds(block * LANES, LANES)]
    ex_ids = pltpu.make_async_remote_copy(ids_mine, ids_buf, ex_send.at[0], ex_recv.at[0], device_id=(stage, other), device_id_type=MESH)
    ex_emb = pltpu.make_async_remote_copy(acc_emb, tab_peer.at[pl.ds(0, vocab)], ex_send.at[1], ex_recv.at[1], device_id=(stage, other), device_id_type=MESH)

    def cot_copy(step_id):
        return pltpu.make_async_remote_copy(dx_send.at[step_id], cot_in.at[step_id], cot_send.at[step_id], cot_recv.at[step_id],
                                            device_id=(jnp.maximum(stage - 1, 0), rep), device_id_type=MESH)

    chunk_rows = d_out.shape[0] // CHUNKS

    def piece(step_id, chunk):
        return dx_all.at[rep, last - step_id, pl.ds(chunk * chunk_rows, chunk_rows)]

    def sent(step_id, chunk):
        return dx_send.at[step_id, pl.ds(chunk * chunk_rows, chunk_rows)]

    def bc_copy(step_id, chunk, target):
        return pltpu.make_async_remote_copy(sent(step_id, chunk), piece(step_id, chunk), bc_send.at[target, step_id, chunk], bc_recv.at[step_id, chunk],
                                            device_id=(target, rep), device_id_type=MESH)

    def relay_copy(step_id, chunk):
        return pltpu.make_async_remote_copy(piece(step_id, chunk), piece(step_id, chunk), bc_send.at[last, step_id, chunk], bc_recv.at[step_id, chunk],
                                            device_id=(last, rep), device_id_type=MESH)

    def peer_copy(step_id, chunk, src):
        return pltpu.make_async_remote_copy(src, piece(step_id, chunk), pr_send.at[step_id, chunk], pr_recv.at[step_id, chunk],
                                            device_id=(stage, other), device_id_type=MESH)

    def local_copy(step_id):
        return pltpu.make_async_copy(dx_send.at[step_id], dx_all.at[rep, last - step_id], loc_sem.at[step_id])

    @pl.loop(0, stages)
    def _(step_id):
        @pl.when(stage + step_id <= last)
        def _():
            forward(step_id)

            @pl.when(step_id == 0)
            def _():
                pl.semaphore_wait(barrier, 2 * stages - 1)
                ex_ids.start()
                ex_emb.start()
                load_in.wait()
                load_out.wait()
                cot[...] = d_out[...]

            @pl.when(step_id > 0)
            def _():
                cot_copy(step_id - 1).wait_recv()
                cot[...] = cot_in[step_id - 1]

            each_layer(layers, tokens, BACKWARD_PARTS, lambda back_id, rows: backward_layer(layers - 1 - back_id, rows, w_half, w_out, acts_x, acts_a, acts_s, cot, sum_in, sum_out_t))
            dx_send[step_id] = cot[...]

            @pl.when(stage > 0)
            def _():
                cot_copy(step_id).start()

            @pl.when(stage == 0)
            def _():
                for first, second in zip(ROUTES[1], ROUTES[2]):
                    bc_copy(step_id, first, 1).start()
                    bc_copy(step_id, second, 2).start()
                for chunk in range(CHUNKS):
                    peer_copy(step_id, chunk, sent(step_id, chunk)).start()
                local_copy(step_id).start()

    ex_ids.wait()
    mark_buf[...] = mark_repeats(ids_mine[...]) | mark_repeats(ids_buf[...])
    small = [
        pltpu.make_async_copy(mark_buf, marks, load_sem.at[3]),
        pltpu.make_async_copy(ids_buf, ids_peer, load_sem.at[4]),
        pltpu.make_async_copy(ids_mine, ids_own, load_sem.at[5]),
    ]
    for copy in small:
        copy.start()

    gi_bf = acts_a.at[:, pl.ds(0, w_in.shape[1]), :]
    go_bf = acts_x.at[pl.ds(0, layers)]

    @pl.loop(0, layers)
    def _(layer_id):
        gi_bf[layer_id] = sum_in[layer_id].astype(BF16)
        go_bf[layer_id] = (sum_out_t[layer_id].T + acc_o[layer_id]).astype(BF16)

    half_i = gi_own.shape[1]
    half_o = go_own.shape[1]
    keep = [
        pltpu.make_async_copy(gi_bf.at[:, pl.ds(pl.multiple_of(rep * half_i, half_i), half_i), :], gi_own, g_sem.at[0]),
        pltpu.make_async_copy(go_bf.at[:, pl.ds(pl.multiple_of(rep * half_o, half_o), half_o), :], go_own, g_sem.at[1]),
    ]
    give = [
        pltpu.make_async_remote_copy(gi_bf.at[:, pl.ds(pl.multiple_of(other * half_i, half_i), half_i), :], gi_recv, g_send.at[0], g_recv.at[0], device_id=(stage, other), device_id_type=MESH),
        pltpu.make_async_remote_copy(go_bf.at[:, pl.ds(pl.multiple_of(other * half_o, half_o), half_o), :], go_recv, g_send.at[1], g_recv.at[1], device_id=(stage, other), device_id_type=MESH),
    ]
    for copy in keep + give:
        copy.start()

    for place, order in ROUTES.items():
        @pl.when(stage == place)
        def _():
            for step_id in range(stages):
                for pos, chunk in enumerate(order):
                    bc_copy(step_id, chunk, 0).wait_recv()
                    if place < last and pos < CHUNKS // 2:
                        relay_copy(step_id, chunk).start()
                    peer_copy(step_id, chunk, piece(step_id, chunk)).start()
            for step_id in range(stages):
                if place < last:
                    for chunk in order[:CHUNKS // 2]:
                        relay_copy(step_id, chunk).wait_send()
                if place + step_id <= last:
                    cot_copy(step_id).wait_send()

    @pl.when(stage == 0)
    def _():
        for step_id in range(stages):
            for chunk in range(CHUNKS):
                for target in (1, 2):
                    bc_copy(step_id, chunk, target).wait_send()
            local_copy(step_id).wait()

    for step_id in range(stages):
        for chunk in range(CHUNKS):
            peer_copy(step_id, chunk, sent(step_id, chunk)).wait()
    for copy in keep + give:
        copy.wait()
    for copy in small:
        copy.wait()
    ex_emb.wait()
    load_emb.wait()


def finish_kernel(ids_own, ids_peer, marks, tab_own, tab_peer, dx_all, gi_own, gi_recv, go_own, go_recv,
                  emb_t, grad_in, grad_out, dxf, gi_buf, go_buf, gi_out, go_out, sems):
    step = pl.program_id(0)
    rep = lax.axis_index('dp')
    padded = tab_own.shape[0]
    width = tab_own.shape[2]
    rows_own = tab_own.reshape(padded, width)
    rows_peer = tab_peer.reshape(padded, width)
    micros = dx_all.shape[1]
    loads = [pltpu.make_async_copy(src, dst, sems.at[pos]) for pos, (src, dst) in enumerate(
        ((gi_own, gi_buf.at[0]), (gi_recv, gi_buf.at[1]), (go_own, go_buf.at[0]), (go_recv, go_buf.at[1])))]
    stores = [pltpu.make_async_copy(gi_out, grad_in, sems.at[4]), pltpu.make_async_copy(go_out, grad_out, sems.at[5])]

    @pl.when(step == 0)
    def _():
        for copy in loads:
            copy.start()
        dxf[0] = dx_all[rep].astype(F32)
        dxf[1] = dx_all[1 - rep].astype(F32)
        sides = ((ids_own, rows_own, 0), (ids_peer, rows_peer, 1))

        @pl.loop(0, ids_own.shape[0])
        def _(line):
            micro = lax.rem(line, micros)
            token = (line // micros) * LANES

            for base in range(0, LANES, GROUP):
                repeated = marks[line, base] != 0

                @pl.when(repeated)
                def _():
                    @pl.loop(0, GROUP)
                    def _(pos):
                        for ids, rows, side in sides:
                            row = pl.ds(ids[line, base + pos], 1)
                            rows[row, :] = rows[row, :] + dxf[side, micro, pl.ds(token + base + pos, 1), :]

                @pl.when(jnp.logical_not(repeated))
                def _():
                    def add_batch(start):
                        sums = []
                        for ids, rows, side in sides:
                            for pos in range(start, start + BATCH):
                                row = pl.ds(ids[line, base + pos], 1)
                                sums.append((rows, row, rows[row, :] + dxf[side, micro, pl.ds(token + base + pos, 1), :]))
                        return sums

                    def store_batch(sums):
                        for rows, row, value in sums:
                            rows[row, :] = value

                    held = add_batch(0)
                    for start in range(BATCH, GROUP, BATCH):
                        fresh = add_batch(start)
                        store_batch(held)
                        held = fresh
                    store_batch(held)

        for copy in loads:
            copy.wait()
        gi_out[...] = (gi_buf[0].astype(F32) + gi_buf[1].astype(F32)) * 0.5
        go_out[...] = (go_buf[0].astype(F32) + go_buf[1].astype(F32)) * 0.5
        for copy in stores:
            copy.start()

    half = emb_t.shape[0]
    row_id = lax.broadcasted_iota(jnp.int32, (half, width), 0)
    col_id = lax.broadcasted_iota(jnp.int32, (half, width), 1)
    pick = jnp.where(lax.rem(col_id, half) == row_id, 0.5, 0.0).astype(BF16)
    mine = lax.broadcasted_iota(jnp.int32, (VOCAB_TILE, width), 1) // half == rep
    for start in range(0, emb_t.shape[1], VOCAB_TILE):
        rows = pl.ds(pl.multiple_of(step * emb_t.shape[1] + start, 8), VOCAB_TILE)
        both = jnp.where(mine, rows_own[rows, :], pltpu.roll(rows_peer[rows, :], half, 1)).astype(BF16)
        emb_t[:, start:start + VOCAB_TILE] = lax.dot_general(pick, both, NT, preferred_element_type=F32)

    @pl.when(step == pl.num_programs(0) - 1)
    def _():
        for copy in stores:
            copy.wait()


def solution(mesh):
    stages = mesh.shape['pp']

    def device_body(tok_ids, d_out, stored_x, w_in, w_out, acc_in, acc_out, acc_emb):
        layers, hid, ff = w_in.shape
        tokens = d_out.shape[1]
        vocab = acc_emb.shape[1]
        half_i, half_o, half_e = hid // 2, ff // 2, hid // 2
        emb_rows = acc_emb.reshape(vocab, 1, hid)
        lines = jax.ShapeDtypeStruct((tok_ids.size // LANES, LANES), tok_ids.dtype)
        table = pltpu.VMEM((pl.cdiv(vocab, VOCAB_BLOCK) * VOCAB_BLOCK, 1, hid), F32)
        any_spec = pl.BlockSpec(memory_space=pltpu.HBM)
        vmem_spec = pl.BlockSpec(memory_space=pltpu.VMEM)
        dma = pltpu.SemaphoreType.DMA
        marks, ids_own, ids_peer, tab_own, tab_peer, dx_all, gi_own, gi_recv, go_own, go_recv = pl.pallas_call(
            functools.partial(stage_kernel, stages),
            name='stage_pipeline',
            in_specs=[vmem_spec] * 5 + [any_spec] * 3,
            out_specs=[any_spec] * 3 + [vmem_spec] * 3 + [any_spec] * 4,
            out_shape=[
                lines,
                lines,
                lines,
                table,
                table,
                pltpu.VMEM((2, stages, tokens, hid), BF16),
                jax.ShapeDtypeStruct((layers, half_i, ff), BF16),
                jax.ShapeDtypeStruct((layers, half_i, ff), BF16),
                jax.ShapeDtypeStruct((layers, half_o, hid), BF16),
                jax.ShapeDtypeStruct((layers, half_o, hid), BF16),
            ],
            scratch_shapes=[
                pltpu.VMEM((layers, hid, ff), BF16),
                pltpu.VMEM((layers + 1, tokens, hid), BF16),
                pltpu.VMEM((layers, tokens, ff), BF16),
                pltpu.VMEM((layers, tokens, ff), F32),
                pltpu.VMEM((tokens, hid), BF16),
                pltpu.VMEM((stages, tokens, hid), BF16),
                pltpu.VMEM((stages, tokens, hid), BF16),
                pltpu.VMEM((layers, hid, ff), F32),
                pltpu.VMEM((layers, hid, ff), F32),
                pltpu.VMEM((layers, ff, hid), F32),
                pltpu.VMEM(lines.shape, jnp.int32),
                pltpu.VMEM(lines.shape, jnp.int32),
                pltpu.VMEM(lines.shape, jnp.int32),
                dma((6,)), dma((2,)), dma((2,)),
                dma((stages,)), dma((stages,)),
                dma((stages, stages, CHUNKS)), dma((stages, CHUNKS)),
                dma((stages, CHUNKS)), dma((stages, CHUNKS)), dma((stages,)),
                dma((2,)), dma((2,)), dma((2,)),
            ],
            compiler_params=pltpu.CompilerParams(collective_id=0, has_side_effects=True, vmem_limit_bytes=30 * 2**20),
        )(tok_ids, d_out[0], stored_x[0], w_in, w_out, acc_in[:, 0], acc_out[:, 0], emb_rows)

        resident = lambda x: pltpu.with_memory_space_constraint(x, pltpu.VMEM)
        smem_spec = pl.BlockSpec(memory_space=pltpu.SMEM)
        emb_t, grad_in, grad_out = pl.pallas_call(
            finish_kernel,
            name='finish',
            grid=(pl.cdiv(vocab, VOCAB_BLOCK),),
            in_specs=[smem_spec] * 3 + [vmem_spec] * 3 + [any_spec] * 4,
            out_specs=[pl.BlockSpec((half_e, VOCAB_BLOCK), lambda step: (0, step))] + [any_spec] * 2,
            out_shape=[
                jax.ShapeDtypeStruct((half_e, vocab), F32),
                jax.ShapeDtypeStruct((layers, half_i, ff), F32),
                jax.ShapeDtypeStruct((layers, half_o, hid), F32),
            ],
            scratch_shapes=[
                pltpu.VMEM((2, stages, tokens, hid), F32),
                pltpu.VMEM((2, layers, half_i, ff), BF16),
                pltpu.VMEM((2, layers, half_o, hid), BF16),
                pltpu.VMEM((layers, half_i, ff), F32),
                pltpu.VMEM((layers, half_o, hid), F32),
                dma((6,)),
            ],
            compiler_params=pltpu.CompilerParams(vmem_limit_bytes=30 * 2**20),
        )(ids_own, ids_peer, marks, resident(tab_own), resident(tab_peer), resident(dx_all), gi_own, gi_recv, go_own, go_recv)
        return grad_in, grad_out, emb_t.T

    return jax.shard_map(device_body, mesh=mesh, in_specs=(P(None, 'dp'), P('pp', 'dp', None), P('pp', None, 'dp', None), P('pp', None, None), P('pp', None, None), P('pp', 'dp', None, None), P('pp', 'dp', None, None), P('dp', None, None)), out_specs=(P('pp', 'dp', None), P('pp', 'dp', None), P(None, 'dp')), check_vma=False)
```
